32 devices in a mesh: face: 2 (over y), fy: 4 (over x, core), fx: 4 (over z).
Axes of the slice: x: 2, y: 2, z: 4, core: 2. Of those that a mesh axis runs over, the one named last changes fastest.
Arguments:
- state: float32 [6, 32, 32, 192], P('face', 'fy', 'fx'), may hold values from -6 to 6
- jacobian: float32 [6, 32, 32], P('face', 'fy', 'fx'), may hold values from 0.5 to 2
- metric_diag: float32 [2, 6, 32, 32], P(None, 'face', 'fy', 'fx'), may hold values from 0.6 to 1.4
- metric_cross: float32 [6, 32, 32], P('face', 'fy', 'fx'), may hold values from -0.3 to 0.3
- coriolis: float32 [6, 32, 32], P('face', 'fy', 'fx'), may hold values from -2 to 2
- nbr_face: int32 [6, 4], replicated, may hold values from 0 to 5, as said below
- nbr_edge: int32 [6, 4], replicated, may hold values from 0 to 3, as said below
Outputs:
- updated: float32 [6, 32, 32, 192], P('face', 'fy', 'fx')
The draws below stay inside these ranges and needn't reach their ends.
Inputs may be any that keep to these rules, and one draw needn't show every extreme that they name: Edge e of a face is 0 south (row 0), 1 east (last column), 2 north (last row), 3 west (column 0). Edge e of face f is glued to edge nbr_edge[f, e] of face nbr_face[f, e], and that edge back to it; the 6 faces are glued as the surface of a cube, three faces at each corner, the two glued edges running in opposite senses when both are read counterclockwise. `nbr_edge`: see nbr_face.
All inputs are finite; a program needn't handle non-finite values.
Results may differ from the reference program's by a relative error of at most 0.0001.
Values sent between devices are 32-bit elements; how exact they have to be, the bound alone decides.
A program may use at most 64 MiB of HBM per device.

```python
import math
import jax
import jax.numpy as jnp
import numpy as np
from jax import lax

FACES = 6
LEV = 64
NN = 32


def glued_tables(key):
    base_key = jax.random.fold_in(key, 4051)
    relabel = jax.random.permutation(jax.random.fold_in(base_key, 1), 6).astype(jnp.int32)
    quarter = jax.random.randint(jax.random.fold_in(base_key, 2), (6,), 0, 4).astype(jnp.int32)
    drawn_face = jnp.asarray(np.array([[5, 1, 4, 3], [5, 2, 4, 0], [5, 3, 4, 1], [5, 0, 4, 2], [0, 1, 2, 3], [2, 1, 0, 3]]), jnp.int32)
    drawn_edge = jnp.asarray(np.array([[2, 3, 0, 1], [1, 3, 1, 1], [0, 3, 2, 1], [3, 3, 3, 1], [2, 2, 2, 2], [0, 0, 0, 0]]), jnp.int32)
    old_face = jnp.broadcast_to(jnp.arange(6, dtype=jnp.int32)[:, None], (6, 4))
    old_edge = jnp.broadcast_to(jnp.arange(4, dtype=jnp.int32)[None, :], (6, 4))
    new_face = relabel[old_face]
    new_edge = (old_edge + quarter[old_face]) % 4
    glued_face = relabel[drawn_face]
    glued_edge = (drawn_edge + quarter[drawn_face]) % 4
    faces_out = jnp.zeros((6, 4), jnp.int32).at[new_face, new_edge].set(glued_face)
    edges_out = jnp.zeros((6, 4), jnp.int32).at[new_face, new_edge].set(glued_edge)
    return (faces_out, edges_out)


def draw_nbr_face(key, part):
    return glued_tables(key)[0]


def draw_nbr_edge(key, part):
    return glued_tables(key)[1]


def level_of(key, shape, pieces, smallest, top_value):
    gain, own = 1.0, jax.random.fold_in(key, 6)
    for axis_at, blocks in pieces:
        draws = jnp.exp(jax.random.uniform(jax.random.fold_in(own, axis_at), (blocks,), jnp.float32, smallest / len(pieces), top_value / len(pieces)))
        gain = gain * jnp.repeat(draws, shape[axis_at] // blocks).reshape([-1 if axis == axis_at else 1 for axis in range(len(shape))])
    return gain


def bell_draw(key, dims, scale, most, split=(), held_as=jnp.bfloat16):
    level = level_of(key, dims, split, -0.22, 0.18) if split else 1.0
    values = jax.random.normal(key, dims, jnp.float32) * scale * level
    return jnp.minimum(jnp.maximum(values, -most), most).astype(held_as)


def setup_inputs(seed: int = 0) -> dict:
    splits = jax.random.split(jax.random.key(seed), 8)
    return {
        "state": bell_draw(splits[0], (FACES, NN, NN, 3 * LEV), 1.0, 6.0, ((0, 2), (1, 4), (2, 4)), jnp.float32),
        "jacobian": jnp.clip(jnp.exp(math.log(2.0) - 1.3862944 * jax.random.uniform(splits[1], (FACES, NN, NN), jnp.float32) ** level_of(splits[1], (FACES, NN, NN), ((0, 2), (1, 4), (2, 4)), -0.2, 0.2)), 0.5, 2.0),
        "metric_diag": jnp.clip(1.0 + 0.08 * jax.random.normal(splits[2], (2, FACES, NN, NN), jnp.float32), 0.6, 1.4),
        "metric_cross": jnp.clip(jax.random.uniform(splits[3], (FACES, NN, NN), jnp.float32, -0.3, 0.3) * level_of(splits[3], (FACES, NN, NN), ((0, 2), (1, 4), (2, 4)), -0.4, 0.0), -0.3, 0.3),
        "coriolis": jnp.clip(jax.random.uniform(splits[4], (FACES, NN, NN), jnp.float32, -2.0, 2.0) * level_of(splits[4], (FACES, NN, NN), ((0, 2), (1, 4), (2, 4)), -0.4, 0.0), -2.0, 2.0),
        "nbr_face": draw_nbr_face(jax.random.fold_in(splits[7], 71), 0),
        "nbr_edge": draw_nbr_edge(jax.random.fold_in(splits[7], 71), 0),
    }


time_step = 0.05
hyper_coeff = 0.0005

def deriv_table():
    gll_nodes = np.array([-1.0, -1.0 / np.sqrt(5.0), 1.0 / np.sqrt(5.0), 1.0])
    bary_weights = np.ones(4)
    for j in range(4):
        for m in range(4):
            if m != j:
                bary_weights[j] = bary_weights[j] / (gll_nodes[j] - gll_nodes[m])
    matrix = np.zeros((4, 4))
    for i in range(4):
        for j in range(4):
            if i != j:
                matrix[i, j] = bary_weights[j] / bary_weights[i] / (gll_nodes[i] - gll_nodes[j])
        matrix[i, i] = -np.sum(matrix[i])
    return matrix

def along_x(values):
    face_count, row_count, col_count, chan_count = values.shape
    blocks = values.reshape(face_count, row_count, col_count // 4, 4, chan_count)
    result = jnp.einsum('jk,abekc->abejc', jnp.asarray(deriv_table(), jnp.float32), blocks, precision=lax.Precision.HIGHEST)
    return result.reshape(values.shape)

def along_y(values):
    face_count, row_count, col_count, chan_count = values.shape
    blocks = values.reshape(face_count, row_count // 4, 4, col_count, chan_count)
    result = jnp.einsum('ik,aekxc->aeixc', jnp.asarray(deriv_table(), jnp.float32), blocks, precision=lax.Precision.HIGHEST)
    return result.reshape(values.shape)

def mass_of(jacobian):
    weights = jnp.asarray([1.0 / 6.0, 5.0 / 6.0, 5.0 / 6.0, 1.0 / 6.0], jnp.float32)
    row_weight = jnp.tile(weights, jacobian.shape[1] // 4)
    col_weight = jnp.tile(weights, jacobian.shape[2] // 4)
    return jacobian * row_weight[None, :, None] * col_weight[None, None, :]

def tendency(state, geometry, planet):
    volume, metric_xx, metric_yy, metric_xy = geometry
    levels = state.shape[-1] // 3
    wind_u = state[..., :levels]
    wind_v = state[..., levels:2 * levels]
    temper = state[..., 2 * levels:]
    contra_u = metric_xx * wind_u + metric_xy * wind_v
    contra_v = metric_xy * wind_u + metric_yy * wind_v
    energy = 0.5 * (wind_u * contra_u + wind_v * contra_v) + temper
    xderivs = along_x(jnp.concatenate([wind_v, temper, energy], -1))
    yderivs = along_y(jnp.concatenate([wind_u, temper, energy], -1))
    absolute = (xderivs[..., :levels] - yderivs[..., :levels]) / volume + planet
    tend_u = absolute * volume * contra_v - xderivs[..., 2 * levels:]
    tend_v = -absolute * volume * contra_u - yderivs[..., 2 * levels:]
    tend_t = -(contra_u * xderivs[..., levels:2 * levels] + contra_v * yderivs[..., levels:2 * levels])
    return state + time_step * jnp.concatenate([tend_u, tend_v, tend_t], -1)

def laplace(values, geometry):
    volume, metric_xx, metric_yy, metric_xy = geometry
    grad_x = along_x(values)
    grad_y = along_y(values)
    flux_x = volume * (metric_xx * grad_x + metric_xy * grad_y)
    flux_y = volume * (metric_xy * grad_x + metric_yy * grad_y)
    return (along_x(flux_x) + along_y(flux_y)) / volume

def combine(values, axis):
    length = values.shape[axis] - 2
    positions = jnp.arange(length)
    leading = (positions % 4 == 0).astype(jnp.float32)
    trailing = (positions % 4 == 3).astype(jnp.float32)
    broad_shape = [1, 1, 1, 1]
    broad_shape[axis] = length
    leading = leading.reshape(broad_shape)
    trailing = trailing.reshape(broad_shape)
    middle = lax.slice_in_dim(values, 1, length + 1, axis=axis)
    previous = lax.slice_in_dim(values, 0, length, axis=axis)
    following = lax.slice_in_dim(values, 2, length + 2, axis=axis)
    return middle + leading * previous + trailing * following

def rotate(segment, quarter, levels):
    cosine = ((quarter == 0).astype(jnp.float32) - (quarter == 2).astype(jnp.float32))[..., None]
    sine_part = ((quarter == 1).astype(jnp.float32) - (quarter == 3).astype(jnp.float32))[..., None]
    wind_u = segment[..., :levels]
    wind_v = segment[..., levels:2 * levels]
    return jnp.concatenate([cosine * wind_u - sine_part * wind_v, sine_part * wind_u + cosine * wind_v, segment[..., 2 * levels:]], -1)

def assemble(values, vector, nbr_face, nbr_edge):
    padded = jnp.pad(values, ((0, 0), (1, 1), (1, 1), (0, 0)))
    summed = combine(combine(padded, 1), 2)
    side_nodes = summed.shape[1]
    levels = summed.shape[-1] // 3
    rim_strips = jnp.stack([summed[:, 0, :], summed[:, :, side_nodes - 1], summed[:, side_nodes - 1, ::-1], summed[:, ::-1, 0]], axis=1)
    partner = rim_strips[nbr_face, nbr_edge][:, :, ::-1]
    if vector:
        quarter = (jnp.arange(4, dtype=jnp.int32)[None, :] - nbr_edge + 2) % 4
        partner = rotate(partner, quarter[:, :, None], levels)
    result = summed.at[:, 0, :].add(partner[:, 0])
    result = result.at[:, :, side_nodes - 1].add(partner[:, 1])
    result = result.at[:, side_nodes - 1, :].add(partner[:, 2, ::-1])
    result = result.at[:, :, 0].add(partner[:, 3, ::-1])
    return result

def reference(state, jacobian, metric_diag, metric_cross, coriolis, nbr_face, nbr_edge):
    node_mass = mass_of(jacobian)[..., None]
    total_mass = assemble(node_mass, False, nbr_face, nbr_edge)
    geometry = (jacobian[..., None], metric_diag[0][..., None], metric_diag[1][..., None], metric_cross[..., None])
    raw = tendency(state, geometry, coriolis[..., None])
    sectioned = assemble(node_mass * raw, True, nbr_face, nbr_edge) / total_mass
    first_lap = assemble(node_mass * laplace(sectioned, geometry), True, nbr_face, nbr_edge) / total_mass
    second_lap = assemble(node_mass * laplace(first_lap, geometry), True, nbr_face, nbr_edge) / total_mass
    return sectioned - hyper_coeff * second_lap
```

```python
import functools

import jax
import jax.numpy as jnp
import numpy as np
from jax import lax
from jax.experimental import pallas as pl
from jax.experimental.pallas import tpu as pltpu
from jax.sharding import PartitionSpec as P

time_step = 0.05
hyper_coeff = 0.0005
MESH = pl.DeviceIdType.MESH
ROUNDS = 3


def padded(cells, sides, width):
    for axis, dim in sides:
        count = lax.axis_size(axis)
        ends = count - 1
        head = lax.slice_in_dim(cells, 0, width, axis=dim)
        tail = lax.slice_in_dim(cells, cells.shape[dim] - width, cells.shape[dim], axis=dim)
        cells = jnp.concatenate(
            [
                lax.ppermute(tail, axis, [(i, (i + 1) % count) for i in range(ends)]),
                cells,
                lax.ppermute(head, axis, [((i + 1) % count, i) for i in range(ends)]),
            ],
            axis=dim,
        )
    return cells


def deriv_table():
    gll_nodes = np.array([-1.0, -1.0 / np.sqrt(5.0), 1.0 / np.sqrt(5.0), 1.0])
    bary_weights = np.ones(4)
    for j in range(4):
        for m in range(4):
            if m != j:
                bary_weights[j] = bary_weights[j] / (gll_nodes[j] - gll_nodes[m])
    matrix = np.zeros((4, 4))
    for i in range(4):
        for j in range(4):
            if i != j:
                matrix[i, j] = bary_weights[j] / bary_weights[i] / (gll_nodes[i] - gll_nodes[j])
        matrix[i, i] = -np.sum(matrix[i])
    return matrix


def along_x(values):
    face_count, row_count, col_count, chan_count = values.shape
    blocks = values.reshape(face_count, row_count, col_count // 4, 4, chan_count)
    result = jnp.einsum(
        "jk,abekc->abejc",
        jnp.asarray(deriv_table(), jnp.float32),
        blocks,
        precision=lax.Precision.HIGHEST,
    )
    return result.reshape(values.shape)


def along_y(values):
    face_count, row_count, col_count, chan_count = values.shape
    blocks = values.reshape(face_count, row_count // 4, 4, col_count, chan_count)
    result = jnp.einsum(
        "ik,aekxc->aeixc",
        jnp.asarray(deriv_table(), jnp.float32),
        blocks,
        precision=lax.Precision.HIGHEST,
    )
    return result.reshape(values.shape)


def mass_of(jacobian):
    weights = jnp.asarray([1.0 / 6.0, 5.0 / 6.0, 5.0 / 6.0, 1.0 / 6.0], jnp.float32)
    row_weight = jnp.tile(weights, jacobian.shape[1] // 4)
    col_weight = jnp.tile(weights, jacobian.shape[2] // 4)
    return jacobian * row_weight[None, :, None] * col_weight[None, None, :]


def tendency(state, geometry, planet):
    volume, metric_xx, metric_yy, metric_xy = geometry
    levels = state.shape[-1] // 3
    wind_u = state[..., :levels]
    wind_v = state[..., levels : 2 * levels]
    temper = state[..., 2 * levels :]
    contra_u = metric_xx * wind_u + metric_xy * wind_v
    contra_v = metric_xy * wind_u + metric_yy * wind_v
    energy = 0.5 * (wind_u * contra_u + wind_v * contra_v) + temper
    xderivs = along_x(jnp.concatenate([wind_v, temper, energy], -1))
    yderivs = along_y(jnp.concatenate([wind_u, temper, energy], -1))
    absolute = (xderivs[..., :levels] - yderivs[..., :levels]) / volume + planet
    tend_u = absolute * volume * contra_v - xderivs[..., 2 * levels :]
    tend_v = -absolute * volume * contra_u - yderivs[..., 2 * levels :]
    tend_t = -(
        contra_u * xderivs[..., levels : 2 * levels] + contra_v * yderivs[..., levels : 2 * levels]
    )
    return state + time_step * jnp.concatenate([tend_u, tend_v, tend_t], -1)


def laplace(values, geometry):
    volume, metric_xx, metric_yy, metric_xy = geometry
    grad_x = along_x(values)
    grad_y = along_y(values)
    flux_x = volume * (metric_xx * grad_x + metric_xy * grad_y)
    flux_y = volume * (metric_xy * grad_x + metric_yy * grad_y)
    return (along_x(flux_x) + along_y(flux_y)) / volume


def combine(values, axis):
    length = values.shape[axis] - 2
    positions = jnp.arange(length)
    leading = (positions % 4 == 0).astype(jnp.float32)
    trailing = (positions % 4 == 3).astype(jnp.float32)
    broad_shape = [1, 1, 1, 1]
    broad_shape[axis] = length
    leading = leading.reshape(broad_shape)
    trailing = trailing.reshape(broad_shape)
    middle = lax.slice_in_dim(values, 1, length + 1, axis=axis)
    previous = lax.slice_in_dim(values, 0, length, axis=axis)
    following = lax.slice_in_dim(values, 2, length + 2, axis=axis)
    return middle + leading * previous + trailing * following


def rotate(segment, quarter, levels):
    cosine = ((quarter == 0).astype(jnp.float32) - (quarter == 2).astype(jnp.float32))[..., None]
    sine_part = ((quarter == 1).astype(jnp.float32) - (quarter == 3).astype(jnp.float32))[..., None]
    wind_u = segment[..., :levels]
    wind_v = segment[..., levels : 2 * levels]
    return jnp.concatenate(
        [
            cosine * wind_u - sine_part * wind_v,
            sine_part * wind_u + cosine * wind_v,
            segment[..., 2 * levels :],
        ],
        -1,
    )


def in_face(values):
    across = combine(padded(values, (("fx", 2),), 1), 2)
    return combine(padded(across, (("fy", 1),), 1), 1)


def place_pieces(
    got_flat,
    got_tall,
    vector,
    nbr_edge,
    flat_edge,
    tall_edge,
    on_south,
    on_west,
    flat_start,
    tall_start,
    face_local,
    side_nodes,
    chan_count,
    levels,
):
    edge_ids = jnp.arange(4, dtype=jnp.int32)
    flat_target = nbr_edge[:, flat_edge]
    tall_target = nbr_edge[:, tall_edge]
    if vector:
        got_flat = rotate(got_flat, ((flat_target - flat_edge + 2) % 4)[None, :, None], levels)
        got_tall = rotate(got_tall, ((tall_target - tall_edge + 2) % 4)[None, :, None], levels)
    got_flat = jnp.where(on_south, got_flat[:, :, ::-1], got_flat)
    got_tall = jnp.where(on_west, got_tall, got_tall[:, :, ::-1])
    flat_pick = (flat_target[:, None] == edge_ids[None, :]).astype(jnp.float32)
    tall_pick = (tall_target[:, None] == edge_ids[None, :]).astype(jnp.float32)
    flat_rims = jnp.einsum("se,gsjc->gejc", flat_pick, got_flat, precision=lax.Precision.HIGHEST)
    tall_rims = jnp.einsum("se,gsjc->gejc", tall_pick, got_tall, precision=lax.Precision.HIGHEST)
    empty_rims = jnp.zeros((face_local, 4, side_nodes, chan_count), jnp.float32)
    rim_strips = lax.dynamic_update_slice(empty_rims, flat_rims, (0, 0, flat_start, 0))
    return rim_strips + lax.dynamic_update_slice(empty_rims, tall_rims, (0, 0, tall_start, 0))


def outgoing(
    summed, nbr_face, face_ids, flat_edge, tall_edge, on_south, on_west, flat_live, tall_live
):
    row_count = summed.shape[1]
    col_count = summed.shape[2]
    all_faces = jnp.arange(nbr_face.shape[0], dtype=jnp.int32)
    flat_piece = jnp.where(on_south, summed[:, 0], summed[:, row_count - 1])
    tall_piece = jnp.where(on_west, summed[:, :, 0], summed[:, :, col_count - 1])
    flat_dest = nbr_face[face_ids, flat_edge]
    tall_dest = nbr_face[face_ids, tall_edge]
    flat_send = ((all_faces[:, None] == flat_dest[None, :]) & flat_live).astype(jnp.float32)
    tall_send = ((all_faces[:, None] == tall_dest[None, :]) & tall_live).astype(jnp.float32)
    return (
        flat_send[:, :, None, None] * flat_piece[None],
        tall_send[:, :, None, None] * tall_piece[None],
    )


def assemble(values, vector, nbr_face, nbr_edge):
    summed = in_face(values)
    face_local, row_count, col_count, chan_count = summed.shape
    levels = chan_count // 3
    row_index = lax.axis_index("fy")
    col_index = lax.axis_index("fx")
    side_nodes = row_count * lax.axis_size("fy")
    face_ids = lax.axis_index("face") * face_local + jnp.arange(face_local, dtype=jnp.int32)
    on_south = row_index == 0
    on_north = row_index == lax.axis_size("fy") - 1
    on_west = col_index == 0
    on_east = col_index == lax.axis_size("fx") - 1
    flat_live = on_south | on_north
    tall_live = on_west | on_east
    flat_edge = jnp.where(on_south, 0, 2).astype(jnp.int32)
    tall_edge = jnp.where(on_west, 3, 1).astype(jnp.int32)
    flat_start = jnp.where(
        on_south, side_nodes - (col_index + 1) * col_count, col_index * col_count
    )
    tall_start = jnp.where(on_west, row_index * row_count, side_nodes - (row_index + 1) * row_count)
    send_flat, send_tall = outgoing(
        summed, nbr_face, face_ids, flat_edge, tall_edge, on_south, on_west, flat_live, tall_live
    )
    got_flat, got_tall = (
        lax.all_to_all(send_flat, "face", split_axis=0, concat_axis=1, tiled=True),
        lax.all_to_all(send_tall, "face", split_axis=0, concat_axis=1, tiled=True),
    )
    rim_strips = place_pieces(
        got_flat,
        got_tall,
        vector,
        nbr_edge,
        flat_edge,
        tall_edge,
        on_south,
        on_west,
        flat_start,
        tall_start,
        face_local,
        side_nodes,
        chan_count,
        levels,
    )
    flat_lines = jnp.stack([rim_strips[:, 0], rim_strips[:, 2, ::-1]], axis=1)
    flat_lines = flat_lines.reshape(face_local, 2, lax.axis_size("fx"), col_count, chan_count)
    tall_lines = jnp.stack([rim_strips[:, 1], rim_strips[:, 3, ::-1]], axis=1)
    tall_lines = tall_lines.reshape(face_local, 2, lax.axis_size("fy"), row_count, chan_count)
    flat_whole = lax.psum(flat_lines, "fy")
    tall_whole = lax.psum(tall_lines, "fx")
    flat_block = lax.psum_scatter(flat_whole, "fx", scatter_dimension=2, tiled=True)
    tall_block = lax.psum_scatter(tall_whole, "fy", scatter_dimension=2, tiled=True)
    flat_add = jnp.where(on_south, flat_block[:, 0, 0], flat_block[:, 1, 0])
    tall_add = jnp.where(on_west, tall_block[:, 1, 0], tall_block[:, 0, 0])
    result = summed.at[:, 0].add(jnp.where(on_south, flat_add, 0.0))
    result = result.at[:, row_count - 1].add(jnp.where(on_north, flat_add, 0.0))
    result = result.at[:, :, 0].add(jnp.where(on_west, tall_add, 0.0))
    result = result.at[:, :, col_count - 1].add(jnp.where(on_east, tall_add, 0.0))
    return result


def per_device(state, jacobian, metric_diag, metric_cross, coriolis, nbr_face, nbr_edge):
    node_mass = mass_of(jacobian)[..., None]
    total_mass = assemble(node_mass, False, nbr_face, nbr_edge)
    geometry = (
        jacobian[..., None],
        metric_diag[0][..., None],
        metric_diag[1][..., None],
        metric_cross[..., None],
    )
    raw = tendency(state, geometry, coriolis[..., None])
    sectioned = assemble(node_mass * raw, True, nbr_face, nbr_edge) / total_mass
    first_lap = (
        assemble(node_mass * laplace(sectioned, geometry), True, nbr_face, nbr_edge) / total_mass
    )
    second_lap = (
        assemble(node_mass * laplace(first_lap, geometry), True, nbr_face, nbr_edge) / total_mass
    )
    return sectioned - hyper_coeff * second_lap


SIDE = 8
HALF = 64


def tile_place(edge, block, blocks):
    return [
        (0, block),
        (block, blocks - 1),
        (blocks - 1, blocks - 1 - block),
        (blocks - 1 - block, 0),
    ][edge]


def kernel(
    groups,
    blocks,
    nbr_face,
    nbr_edge,
    state,
    jac,
    diag,
    cross,
    coriolis,
    out,
    *scratch,
):
    faces = state.shape[0]
    fields, cols, packs, got_col, got_row, got_pack, rim_0, rim_1, end_0, end_1 = (
        scratch[i * ROUNDS : (i + 1) * ROUNDS] for i in range(10)
    )
    got_rim = [pair for pair in zip(rim_0, rim_1)]
    got_end = [pair for pair in zip(end_0, end_1)]
    (summed, inverse, flux_a, flux_b, flux_c, sem_s_near, sem_r_near, sem_s_rim, sem_r_rim, sem_s_end, sem_r_end) = scratch[
        10 * ROUNDS :
    ]
    g = lax.axis_index("face")
    y = lax.axis_index("fy")
    x = lax.axis_index("fx")
    last = blocks - 1

    barrier = pltpu.get_barrier_semaphore()
    for tg in range(groups):
        for ty in range(blocks):
            for tx in range(blocks):

                @pl.when(jnp.logical_not((g == tg) & (y == ty) & (x == tx)))
                def _():
                    pl.semaphore_signal(barrier, inc=1, device_id=(tg, ty, tx), device_id_type=MESH)

    live = ((y == 0) | (y == last), (x == 0) | (x == last))
    edge = (jnp.where(y == 0, 0, 2), jnp.where(x == 0, 3, 1))
    place = (jnp.where(y == 0, x, last - x), jnp.where(x == 0, last - y, y))
    at_end = (jnp.where(y == 0, 0, SIDE - 1), jnp.where(x == 0, 0, SIDE - 1))
    side = (jnp.where(y == 0, 0, 1), jnp.where(x == 0, 0, 1))
    head_pack = (jnp.where(y == 0, 0, 3), jnp.where(x == 0, 2, 1))
    tail_pack = (jnp.where(y == 0, 1, 2), jnp.where(x == 0, 0, 3))

    near = [(0, -1), (0, 1), (-1, 0), (1, 0), (-1, -1), (-1, 1), (1, -1), (1, 1)]

    def has(dy, dx):
        ok = None
        for d, at in ((dy, y), (dx, x)):
            if d:
                one = at > 0 if d < 0 else at < last
                ok = one if ok is None else ok & one
        return ok

    def near_copy(rnd, n):
        dy, dx = near[n]
        back = near.index((-dy, -dx))
        if dy == 0:
            w = (dx + 1) // 2
            src, dst = cols[rnd].at[w], got_col[rnd].at[1 - w]
        elif dx == 0:
            w = (dy + 1) // 2
            src, dst = fields[rnd].at[:, :, w * (SIDE - 1)], got_row[rnd].at[1 - w]
        else:
            w = (dy + 1) + (dx + 1) // 2
            src, dst = packs[rnd].at[w], got_pack[rnd].at[3 - w]
        return pltpu.make_async_remote_copy(
            src_ref=src,
            dst_ref=dst,
            send_sem=sem_s_near.at[n],
            recv_sem=sem_r_near.at[rnd, back],
            device_id=(g, y + dy, x + dx),
            device_id_type=MESH,
        )

    def near_wait(rnd, n):
        dy, dx = near[n]
        if dy == 0:
            ref = got_col[rnd].at[(dx + 1) // 2]
        elif dx == 0:
            ref = got_row[rnd].at[(dy + 1) // 2]
        else:
            ref = got_pack[rnd].at[(dy + 1) + (dx + 1) // 2]
        return pltpu.make_async_remote_copy(
            src_ref=ref,
            dst_ref=ref,
            send_sem=sem_s_near.at[n],
            recv_sem=sem_r_near.at[rnd, n],
            device_id=(g, y + dy, x + dx),
            device_id_type=MESH,
        )

    def is_me(tg, ty, tx):
        return (g == tg) & (y == ty) & (x == tx)

    def rim_piece(rnd, kind):
        if kind == 0:
            return fields[rnd].at[:, :, at_end[0]]
        return cols[rnd].at[side[1]]

    def each_rim(kind, visit):
        for which, off in ((0, 0), (1, 1), (2, -1)):
            block = last - place[kind] + off
            fits = live[kind] & (block >= 0) & (block <= last)
            block = jnp.clip(block, 0, last)
            for e2 in range(4):
                ty, tx = tile_place(e2, block, blocks)
                for g2 in range(groups):
                    visit(which, e2, g2, (g2, ty, tx), fits)

    def rim_send(rnd, kind):
        def visit(which, e2, g2, target, ok):
            mine = is_me(*target)
            if which == 0:
                src = rim_piece(rnd, kind)
                dst = got_rim[rnd][e2 % 2].at[edge[kind], g]
                send, recv = sem_s_rim.at[kind, e2, g2], sem_r_rim.at[rnd, e2 % 2, edge[kind], g]
            else:
                src = packs[rnd].at[head_pack[kind] if which == 1 else tail_pack[kind]]
                dst = got_end[rnd][e2 % 2].at[which - 1, edge[kind], g]
                send = sem_s_end.at[kind, which - 1, e2, g2]
                recv = sem_r_end.at[rnd, e2 % 2, which - 1, edge[kind], g]

            @pl.when(ok & jnp.logical_not(mine))
            def _():
                pltpu.make_async_remote_copy(
                    src_ref=src, dst_ref=dst, send_sem=send, recv_sem=recv, device_id=target, device_id_type=MESH
                ).start()

            @pl.when(ok & mine)
            def _():
                dst[...] = src[...]

        each_rim(kind, visit)

    def rim_wait_send(rnd, kind):
        def visit(which, e2, g2, target, ok):
            if which == 0:
                src = rim_piece(rnd, kind)
                send, recv = sem_s_rim.at[kind, e2, g2], sem_r_rim.at[rnd, e2 % 2, edge[kind], g]
            else:
                src = packs[rnd].at[head_pack[kind] if which == 1 else tail_pack[kind]]
                send = sem_s_end.at[kind, which - 1, e2, g2]
                recv = sem_r_end.at[rnd, e2 % 2, which - 1, edge[kind], g]

            @pl.when(ok & jnp.logical_not(is_me(*target)))
            def _():
                pltpu.make_async_remote_copy(
                    src_ref=src, dst_ref=src, send_sem=send, recv_sem=recv, device_id=target, device_id_type=MESH
                ).wait_send()

        each_rim(kind, visit)

    def rim_wait(rnd, kind):
        def visit(which, e2, g2, source, ok):
            if which == 0:
                ref = got_rim[rnd][kind].at[e2, g2]
                send, recv = sem_s_rim.at[kind, e2, g2], sem_r_rim.at[rnd, kind, e2, g2]
            else:
                ref = got_end[rnd][kind].at[which - 1, e2, g2]
                send, recv = sem_s_end.at[kind, which - 1, e2, g2], sem_r_end.at[rnd, kind, which - 1, e2, g2]

            @pl.when(ok & jnp.logical_not(is_me(*source)))
            def _():
                pltpu.make_async_remote_copy(
                    src_ref=ref, dst_ref=ref, send_sem=send, recv_sem=recv, device_id=source, device_id_type=MESH
                ).wait_recv()

        each_rim(kind, visit)

    sub = lax.broadcasted_iota(jnp.int32, (SIDE, 128), 0)
    lane = lax.broadcasted_iota(jnp.int32, (SIDE, 128), 1)
    low = lane < HALF
    node = sub % 4
    table = deriv_table()
    weights = (1.0 / 6.0, 5.0 / 6.0, 5.0 / 6.0, 1.0 / 6.0)
    zero = jnp.zeros((SIDE, 128), jnp.float32)

    def per_node(entries):
        total = jnp.full((SIDE, 128), entries[0], jnp.float32)
        for j in range(1, 4):
            total = jnp.where(node == j, jnp.float32(entries[j]), total)
        return total

    col_weight = per_node(weights)
    taps = {
        s: per_node([float(table[j, j + s]) if 0 <= j + s < 4 else 0.0 for j in range(4)])
        for s in range(-3, 4)
    }

    def roll_rows(v, shift):
        return pltpu.roll(v, (-shift) % SIDE, 0)

    def swap(v):
        return pltpu.roll(v, HALF, 1)

    def dx(v):
        total = taps[0] * v
        for s in (-3, -2, -1, 1, 2, 3):
            total = total + taps[s] * roll_rows(v, s)
        return total

    def dy(rows):
        return [sum(jnp.float32(table[i, k]) * rows[k] for k in range(4)) for i in range(4)]

    def join(v):
        return v + jnp.where(sub == 3, roll_rows(v, 1), zero) + jnp.where(sub == 4, roll_rows(v, -1), zero)

    def wide(ref, index, r):
        row = jnp.broadcast_to(ref[index + (pl.ds(r, 1), slice(None))].reshape(1, SIDE), (SIDE, SIDE))
        eye = lax.broadcasted_iota(jnp.int32, (SIDE, SIDE), 0) == lax.broadcasted_iota(jnp.int32, (SIDE, SIDE), 1)
        return jnp.broadcast_to(jnp.sum(jnp.where(eye, row, 0.0), axis=1, keepdims=True), (SIDE, 128))

    def store_field(rnd, part, f, above, rows):
        kept = []
        for e_row, values in enumerate(rows):
            kept.append([join(v) for v in values])
        for e_row in range(len(kept) - 1):
            both = kept[e_row][3] + kept[e_row + 1][0]
            kept[e_row][3] = both
            kept[e_row + 1][0] = both
        flat = [v for values in kept for v in values]
        for r, v in enumerate(flat):
            fields[rnd][part, f, r] = v
            cols[rnd][0, part, f, pl.ds(r, 1)] = v[0:1]
            cols[rnd][1, part, f, pl.ds(r, 1)] = v[SIDE - 1 : SIDE]
        for w in range(4):
            v = flat[(SIDE - 1) * (w // 2)]
            c = (SIDE - 1) * (w % 2)
            packs[rnd][w, pl.ds(part * faces + f, 1)] = v[c : c + 1]

    def exchange(rnd):
        for n, (dy_, dx_) in enumerate(near):

            @pl.when(has(dy_, dx_))
            def _():
                near_copy(rnd, n).start()

        for kind in range(2):
            rim_send(rnd, kind)

        for n, (dy_, dx_) in enumerate(near):
            ok = has(dy_, dx_)
            if dy_ == 0:
                ref = got_col[rnd].at[(dx_ + 1) // 2]
            elif dx_ == 0:
                ref = got_row[rnd].at[(dy_ + 1) // 2]
            else:
                ref = got_pack[rnd].at[(dy_ + 1) + (dx_ + 1) // 2]

            @pl.when(ok)
            def _():
                near_wait(rnd, n).wait_recv()

            @pl.when(jnp.logical_not(ok))
            def _():
                ref[...] = jnp.zeros(ref.shape, jnp.float32)

        for part in range(2):
            for f in range(faces):
                for r in range(SIDE):
                    v = fields[rnd][part, f, r]
                    west = jnp.broadcast_to(got_col[rnd][0, part, f, pl.ds(r, 1)], (SIDE, 128))
                    east = jnp.broadcast_to(got_col[rnd][1, part, f, pl.ds(r, 1)], (SIDE, 128))
                    if r in (0, SIDE - 1):
                        w = 0 if r == 0 else 1
                        v = v + got_row[rnd][w, part, f]
                        west = west + jnp.broadcast_to(got_pack[rnd][2 * w, pl.ds(part * faces + f, 1)], (SIDE, 128))
                        east = east + jnp.broadcast_to(got_pack[rnd][2 * w + 1, pl.ds(part * faces + f, 1)], (SIDE, 128))
                    summed[part, f, r] = v + jnp.where(sub == 0, west, jnp.where(sub == SIDE - 1, east, zero))

        for kind in range(2):
            rim_wait(rnd, kind)
            has_head = place[kind] > 0
            has_tail = place[kind] < last
            first_at = jnp.where(edge[kind] >= 2, SIDE - 1, 0)

            @pl.when(live[kind] & jnp.logical_not(has_head))
            def _():
                got_end[rnd][kind][0] = jnp.zeros(got_end[rnd][kind].shape[1:], jnp.float32)

            @pl.when(live[kind] & jnp.logical_not(has_tail))
            def _():
                got_end[rnd][kind][1] = jnp.zeros(got_end[rnd][kind].shape[1:], jnp.float32)

            @pl.when(live[kind])
            def _():
                for f in range(faces):
                    nf = nbr_face[g * faces + f, edge[kind]]
                    ne = nbr_edge[g * faces + f, edge[kind]]
                    ng, nl = nf // faces, nf % faces
                    quarter = (edge[kind] - ne + 2) % 4
                    cosine = jnp.where(quarter == 0, 1.0, jnp.where(quarter == 2, -1.0, 0.0))
                    sine = jnp.where(quarter == 1, 1.0, jnp.where(quarter == 3, -1.0, 0.0))
                    sine = jnp.where(low, -sine, sine)
                    turned = (1 + jnp.where(edge[kind] >= 2, 1, 0) + jnp.where(ne >= 2, 1, 0)) % 2
                    for part in range(2):
                        rim = got_rim[rnd][kind][ne, ng, part, nl]
                        ends = []
                        for which in range(2):
                            at = part * faces + nl
                            ends.append(
                                jnp.broadcast_to(got_end[rnd][kind][which, ne, ng, pl.ds(at, 1)], (SIDE, 128))
                            )
                        b = jnp.where(sub % 2 == 0, roll_rows(rim, 1), roll_rows(rim, -1))
                        b = jnp.where(sub % 4 < 2, roll_rows(b, 2), roll_rows(b, -2))
                        b = pltpu.roll(b, 4, 0)
                        rim = jnp.where(turned == 1, b, rim)
                        rim = rim + jnp.where(sub == first_at, ends[0], jnp.where(sub == SIDE - 1 - first_at, ends[1], zero))
                        if part == 0:
                            rim = cosine * rim + sine * swap(rim)
                        if kind == 0:
                            summed[part, f, at_end[0]] += rim
                        else:
                            for r in range(SIDE):
                                summed[part, f, r] += jnp.where(
                                    sub == at_end[1], jnp.broadcast_to(rim[r : r + 1], (SIDE, 128)), zero
                                )

        for n, (dy_, dx_) in enumerate(near):

            @pl.when(has(dy_, dx_))
            def _():
                near_copy(rnd, n).wait_send()

        for kind in range(2):
            rim_wait_send(rnd, kind)

    for f in range(faces):
        a_rows, b_rows = [], []
        for e_row in range(SIDE // 4):
            rows = range(4 * e_row, 4 * e_row + 4)
            wind, temp, contra, energy, vol, cor, mass = [], [], [], [], [], [], []
            for r in rows:
                j = wide(jac, (f,), r)
                m_xx, m_yy, m_xy = wide(diag, (0, f), r), wide(diag, (1, f), r), wide(cross, (f,), r)
                flux_a[f, r] = j * m_xx
                flux_b[f, r] = j * m_xy
                flux_c[f, r] = j * m_yy
                w = state[f, r, :, 0 : 2 * HALF]
                t = state[f, r, :, 2 * HALF : 3 * HALF]
                t = jnp.concatenate([t, t], axis=1)
                c = jnp.where(low, m_xx, m_yy) * w + m_xy * swap(w)
                p = w * c
                wind.append(w)
                temp.append(t)
                contra.append(c)
                energy.append(0.5 * (p + swap(p)) + t)
                vol.append(j)
                cor.append(wide(coriolis, (f,), r))
                mass.append(j * (jnp.float32(weights[r % 4]) * col_weight))
            dxs = [dx(jnp.where(low, energy[i], wind[i])) for i in range(4)]
            dys = dy([jnp.where(low, wind[i], energy[i]) for i in range(4)])
            dxt = [dx(temp[i]) for i in range(4)]
            dyt = dy(temp)
            a_out, b_out = [], []
            for i in range(4):
                dxv = jnp.where(low, swap(dxs[i]), dxs[i])
                dyu = jnp.where(low, dys[i], swap(dys[i]))
                spin = (dxv - dyu) + cor[i] * vol[i]
                spin = jnp.where(low, spin, -spin)
                tend = spin * swap(contra[i]) - jnp.where(low, dxs[i], dys[i])
                a_out.append(mass[i] * (wind[i] + time_step * tend))
                q = contra[i] * jnp.where(low, dxt[i], dyt[i])
                b_out.append(mass[i] * jnp.where(low, temp[i] - time_step * (q + swap(q)), 1.0))
            a_rows.append(a_out)
            b_rows.append(b_out)
        store_field(0, 0, f, None, a_rows)
        store_field(0, 1, f, None, b_rows)

    pl.semaphore_wait(barrier, groups * blocks * blocks - 1)
    exchange(0)

    def laplacian(rnd, source):
        for f in range(faces):
            for part in range(2):
                out_rows = []
                for e_row in range(SIDE // 4):
                    rows = range(4 * e_row, 4 * e_row + 4)
                    values = [source(part, f, r) for r in rows]
                    gx = [dx(v) for v in values]
                    gy = dy(values)
                    fx = [flux_a[f, r] * gx[i] + flux_b[f, r] * gy[i] for i, r in enumerate(rows)]
                    fy = [flux_b[f, r] * gx[i] + flux_c[f, r] * gy[i] for i, r in enumerate(rows)]
                    fyy = dy(fy)
                    out_rows.append(
                        [(jnp.float32(weights[i]) * col_weight) * (dx(fx[i]) + fyy[i]) for i in range(4)]
                    )
                store_field(rnd, part, f, None, out_rows)

    for f in range(faces):
        for r in range(SIDE):
            b = summed[1, f, r]
            inv = 1.0 / jnp.where(low, swap(b), b)
            inverse[f, r] = inv
            out[f, r, :, 0 : 2 * HALF] = summed[0, f, r] * inv
            out[f, r, :, 2 * HALF : 3 * HALF] = (b * inv)[:, 0:HALF]
            summed[0, f, r] = summed[0, f, r] * inv
            summed[1, f, r] = b * inv
    laplacian(1, lambda part, f, r: summed[part, f, r])
    exchange(1)
    laplacian(2, lambda part, f, r: summed[part, f, r] * inverse[f, r])
    exchange(2)
    for f in range(faces):
        for r in range(SIDE):
            scale = hyper_coeff * inverse[f, r]
            out[f, r, :, 0 : 2 * HALF] = out[f, r, :, 0 : 2 * HALF] - scale * summed[0, f, r]
            out[f, r, :, 2 * HALF : 3 * HALF] = (
                out[f, r, :, 2 * HALF : 3 * HALF] - (scale * summed[1, f, r])[:, 0:HALF]
            )


def fused(groups, blocks, state, jacobian, metric_diag, metric_cross, coriolis, nbr_face, nbr_edge):
    faces = state.shape[0]
    piece = (2, faces, SIDE, 128)
    tile = (faces, SIDE, SIDE, 128)

    def per_round(shape):
        return [pltpu.VMEM(shape, jnp.float32)] * ROUNDS

    scratch = (
        per_round((2,) + tile)
        + per_round((2,) + piece)
        + per_round((4, SIDE, 128))
        + per_round((2,) + piece)
        + per_round((2,) + piece)
        + per_round((4, SIDE, 128))
        + per_round((4, groups) + piece) * 2
        + per_round((2, 4, groups, SIDE, 128)) * 2
        + [pltpu.VMEM((2,) + tile, jnp.float32)]
        + [pltpu.VMEM(tile, jnp.float32)] * 4
        + [
            pltpu.SemaphoreType.DMA((8,)),
            pltpu.SemaphoreType.DMA((ROUNDS, 8)),
            pltpu.SemaphoreType.DMA((2, 4, groups)),
            pltpu.SemaphoreType.DMA((ROUNDS, 2, 4, groups)),
            pltpu.SemaphoreType.DMA((2, 2, 4, groups)),
            pltpu.SemaphoreType.DMA((ROUNDS, 2, 2, 4, groups)),
        ]
    )
    vmem, smem = pl.BlockSpec(memory_space=pltpu.VMEM), pl.BlockSpec(memory_space=pltpu.SMEM)
    return pl.pallas_call(
        functools.partial(kernel, groups, blocks),
        out_shape=jax.ShapeDtypeStruct(state.shape, jnp.float32),
        in_specs=[smem, smem] + [vmem] * 5,
        out_specs=vmem,
        scratch_shapes=scratch,
        compiler_params=pltpu.CompilerParams(collective_id=0, has_side_effects=True),
    )(nbr_face, nbr_edge, state, jacobian, metric_diag, metric_cross, coriolis)


def solution(mesh):
    groups, rows, columns = (mesh.shape[axis] for axis in ("face", "fy", "fx"))

    def body(*args):
        state = args[0]
        faces = state.shape[0]
        if rows == columns and rows > 1 and state.shape[1:] == (SIDE, SIDE, 3 * HALF) and 2 * faces <= SIDE:
            return fused(groups, rows, *args)
        return per_device(*args)

    return jax.shard_map(
        body,
        mesh=mesh,
        in_specs=(
            P("face", "fy", "fx", None),
            P("face", "fy", "fx"),
            P(None, "face", "fy", "fx"),
            P("face", "fy", "fx"),
            P("face", "fy", "fx"),
            P(),
            P(),
        ),
        out_specs=P("face", "fy", "fx", None),
        check_vma=False,
    )
```

```python
import functools

import jax
import jax.numpy as jnp
import numpy as np
from jax import lax
from jax.experimental import pallas as pl
from jax.experimental.pallas import tpu as pltpu
from jax.sharding import PartitionSpec as P

time_step = 0.05
hyper_coeff = 0.0005
MESH = pl.DeviceIdType.MESH
ROUNDS = 3


def padded(cells, sides, width):
    for axis, dim in sides:
        count = lax.axis_size(axis)
        ends = count - 1
        head = lax.slice_in_dim(cells, 0, width, axis=dim)
        tail = lax.slice_in_dim(cells, cells.shape[dim] - width, cells.shape[dim], axis=dim)
        cells = jnp.concatenate(
            [
                lax.ppermute(tail, axis, [(i, (i + 1) % count) for i in range(ends)]),
                cells,
                lax.ppermute(head, axis, [((i + 1) % count, i) for i in range(ends)]),
            ],
            axis=dim,
        )
    return cells


def deriv_table():
    gll_nodes = np.array([-1.0, -1.0 / np.sqrt(5.0), 1.0 / np.sqrt(5.0), 1.0])
    bary_weights = np.ones(4)
    for j in range(4):
        for m in range(4):
            if m != j:
                bary_weights[j] = bary_weights[j] / (gll_nodes[j] - gll_nodes[m])
    matrix = np.zeros((4, 4))
    for i in range(4):
        for j in range(4):
            if i != j:
                matrix[i, j] = bary_weights[j] / bary_weights[i] / (gll_nodes[i] - gll_nodes[j])
        matrix[i, i] = -np.sum(matrix[i])
    return matrix


def along_x(values):
    face_count, row_count, col_count, chan_count = values.shape
    blocks = values.reshape(face_count, row_count, col_count // 4, 4, chan_count)
    result = jnp.einsum(
        "jk,abekc->abejc",
        jnp.asarray(deriv_table(), jnp.float32),
        blocks,
        precision=lax.Precision.HIGHEST,
    )
    return result.reshape(values.shape)


def along_y(values):
    face_count, row_count, col_count, chan_count = values.shape
    blocks = values.reshape(face_count, row_count // 4, 4, col_count, chan_count)
    result = jnp.einsum(
        "ik,aekxc->aeixc",
        jnp.asarray(deriv_table(), jnp.float32),
        blocks,
        precision=lax.Precision.HIGHEST,
    )
    return result.reshape(values.shape)


def mass_of(jacobian):
    weights = jnp.asarray([1.0 / 6.0, 5.0 / 6.0, 5.0 / 6.0, 1.0 / 6.0], jnp.float32)
    row_weight = jnp.tile(weights, jacobian.shape[1] // 4)
    col_weight = jnp.tile(weights, jacobian.shape[2] // 4)
    return jacobian * row_weight[None, :, None] * col_weight[None, None, :]


def tendency(state, geometry, planet):
    volume, metric_xx, metric_yy, metric_xy = geometry
    levels = state.shape[-1] // 3
    wind_u = state[..., :levels]
    wind_v = state[..., levels : 2 * levels]
    temper = state[..., 2 * levels :]
    contra_u = metric_xx * wind_u + metric_xy * wind_v
    contra_v = metric_xy * wind_u + metric_yy * wind_v
    energy = 0.5 * (wind_u * contra_u + wind_v * contra_v) + temper
    xderivs = along_x(jnp.concatenate([wind_v, temper, energy], -1))
    yderivs = along_y(jnp.concatenate([wind_u, temper, energy], -1))
    absolute = (xderivs[..., :levels] - yderivs[..., :levels]) / volume + planet
    tend_u = absolute * volume * contra_v - xderivs[..., 2 * levels :]
    tend_v = -absolute * volume * contra_u - yderivs[..., 2 * levels :]
    tend_t = -(
        contra_u * xderivs[..., levels : 2 * levels] + contra_v * yderivs[..., levels : 2 * levels]
    )
    return state + time_step * jnp.concatenate([tend_u, tend_v, tend_t], -1)


def laplace(values, geometry):
    volume, metric_xx, metric_yy, metric_xy = geometry
    grad_x = along_x(values)
    grad_y = along_y(values)
    flux_x = volume * (metric_xx * grad_x + metric_xy * grad_y)
    flux_y = volume * (metric_xy * grad_x + metric_yy * grad_y)
    return (along_x(flux_x) + along_y(flux_y)) / volume


def combine(values, axis):
    length = values.shape[axis] - 2
    positions = jnp.arange(length)
    leading = (positions % 4 == 0).astype(jnp.float32)
    trailing = (positions % 4 == 3).astype(jnp.float32)
    broad_shape = [1, 1, 1, 1]
    broad_shape[axis] = length
    leading = leading.reshape(broad_shape)
    trailing = trailing.reshape(broad_shape)
    middle = lax.slice_in_dim(values, 1, length + 1, axis=axis)
    previous = lax.slice_in_dim(values, 0, length, axis=axis)
    following = lax.slice_in_dim(values, 2, length + 2, axis=axis)
    return middle + leading * previous + trailing * following


def rotate(segment, quarter, levels):
    cosine = ((quarter == 0).astype(jnp.float32) - (quarter == 2).astype(jnp.float32))[..., None]
    sine_part = ((quarter == 1).astype(jnp.float32) - (quarter == 3).astype(jnp.float32))[..., None]
    wind_u = segment[..., :levels]
    wind_v = segment[..., levels : 2 * levels]
    return jnp.concatenate(
        [
            cosine * wind_u - sine_part * wind_v,
            sine_part * wind_u + cosine * wind_v,
            segment[..., 2 * levels :],
        ],
        -1,
    )


def in_face(values):
    across = combine(padded(values, (("fx", 2),), 1), 2)
    return combine(padded(across, (("fy", 1),), 1), 1)


def place_pieces(
    got_flat,
    got_tall,
    vector,
    nbr_edge,
    flat_edge,
    tall_edge,
    on_south,
    on_west,
    flat_start,
    tall_start,
    face_local,
    side_nodes,
    chan_count,
    levels,
):
    edge_ids = jnp.arange(4, dtype=jnp.int32)
    flat_target = nbr_edge[:, flat_edge]
    tall_target = nbr_edge[:, tall_edge]
    if vector:
        got_flat = rotate(got_flat, ((flat_target - flat_edge + 2) % 4)[None, :, None], levels)
        got_tall = rotate(got_tall, ((tall_target - tall_edge + 2) % 4)[None, :, None], levels)
    got_flat = jnp.where(on_south, got_flat[:, :, ::-1], got_flat)
    got_tall = jnp.where(on_west, got_tall, got_tall[:, :, ::-1])
    flat_pick = (flat_target[:, None] == edge_ids[None, :]).astype(jnp.float32)
    tall_pick = (tall_target[:, None] == edge_ids[None, :]).astype(jnp.float32)
    flat_rims = jnp.einsum("se,gsjc->gejc", flat_pick, got_flat, precision=lax.Precision.HIGHEST)
    tall_rims = jnp.einsum("se,gsjc->gejc", tall_pick, got_tall, precision=lax.Precision.HIGHEST)
    empty_rims = jnp.zeros((face_local, 4, side_nodes, chan_count), jnp.float32)
    rim_strips = lax.dynamic_update_slice(empty_rims, flat_rims, (0, 0, flat_start, 0))
    return rim_strips + lax.dynamic_update_slice(empty_rims, tall_rims, (0, 0, tall_start, 0))


def outgoing(
    summed, nbr_face, face_ids, flat_edge, tall_edge, on_south, on_west, flat_live, tall_live
):
    row_count = summed.shape[1]
    col_count = summed.shape[2]
    all_faces = jnp.arange(nbr_face.shape[0], dtype=jnp.int32)
    flat_piece = jnp.where(on_south, summed[:, 0], summed[:, row_count - 1])
    tall_piece = jnp.where(on_west, summed[:, :, 0], summed[:, :, col_count - 1])
    flat_dest = nbr_face[face_ids, flat_edge]
    tall_dest = nbr_face[face_ids, tall_edge]
    flat_send = ((all_faces[:, None] == flat_dest[None, :]) & flat_live).astype(jnp.float32)
    tall_send = ((all_faces[:, None] == tall_dest[None, :]) & tall_live).astype(jnp.float32)
    return (
        flat_send[:, :, None, None] * flat_piece[None],
        tall_send[:, :, None, None] * tall_piece[None],
    )


def assemble(values, vector, nbr_face, nbr_edge):
    summed = in_face(values)
    face_local, row_count, col_count, chan_count = summed.shape
    levels = chan_count // 3
    row_index = lax.axis_index("fy")
    col_index = lax.axis_index("fx")
    side_nodes = row_count * lax.axis_size("fy")
    face_ids = lax.axis_index("face") * face_local + jnp.arange(face_local, dtype=jnp.int32)
    on_south = row_index == 0
    on_north = row_index == lax.axis_size("fy") - 1
    on_west = col_index == 0
    on_east = col_index == lax.axis_size("fx") - 1
    flat_live = on_south | on_north
    tall_live = on_west | on_east
    flat_edge = jnp.where(on_south, 0, 2).astype(jnp.int32)
    tall_edge = jnp.where(on_west, 3, 1).astype(jnp.int32)
    flat_start = jnp.where(
        on_south, side_nodes - (col_index + 1) * col_count, col_index * col_count
    )
    tall_start = jnp.where(on_west, row_index * row_count, side_nodes - (row_index + 1) * row_count)
    send_flat, send_tall = outgoing(
        summed, nbr_face, face_ids, flat_edge, tall_edge, on_south, on_west, flat_live, tall_live
    )
    got_flat, got_tall = (
        lax.all_to_all(send_flat, "face", split_axis=0, concat_axis=1, tiled=True),
        lax.all_to_all(send_tall, "face", split_axis=0, concat_axis=1, tiled=True),
    )
    rim_strips = place_pieces(
        got_flat,
        got_tall,
        vector,
        nbr_edge,
        flat_edge,
        tall_edge,
        on_south,
        on_west,
        flat_start,
        tall_start,
        face_local,
        side_nodes,
        chan_count,
        levels,
    )
    flat_lines = jnp.stack([rim_strips[:, 0], rim_strips[:, 2, ::-1]], axis=1)
    flat_lines = flat_lines.reshape(face_local, 2, lax.axis_size("fx"), col_count, chan_count)
    tall_lines = jnp.stack([rim_strips[:, 1], rim_strips[:, 3, ::-1]], axis=1)
    tall_lines = tall_lines.reshape(face_local, 2, lax.axis_size("fy"), row_count, chan_count)
    flat_whole = lax.psum(flat_lines, "fy")
    tall_whole = lax.psum(tall_lines, "fx")
    flat_block = lax.psum_scatter(flat_whole, "fx", scatter_dimension=2, tiled=True)
    tall_block = lax.psum_scatter(tall_whole, "fy", scatter_dimension=2, tiled=True)
    flat_add = jnp.where(on_south, flat_block[:, 0, 0], flat_block[:, 1, 0])
    tall_add = jnp.where(on_west, tall_block[:, 1, 0], tall_block[:, 0, 0])
    result = summed.at[:, 0].add(jnp.where(on_south, flat_add, 0.0))
    result = result.at[:, row_count - 1].add(jnp.where(on_north, flat_add, 0.0))
    result = result.at[:, :, 0].add(jnp.where(on_west, tall_add, 0.0))
    result = result.at[:, :, col_count - 1].add(jnp.where(on_east, tall_add, 0.0))
    return result


def per_device(state, jacobian, metric_diag, metric_cross, coriolis, nbr_face, nbr_edge):
    node_mass = mass_of(jacobian)[..., None]
    total_mass = assemble(node_mass, False, nbr_face, nbr_edge)
    geometry = (
        jacobian[..., None],
        metric_diag[0][..., None],
        metric_diag[1][..., None],
        metric_cross[..., None],
    )
    raw = tendency(state, geometry, coriolis[..., None])
    sectioned = assemble(node_mass * raw, True, nbr_face, nbr_edge) / total_mass
    first_lap = (
        assemble(node_mass * laplace(sectioned, geometry), True, nbr_face, nbr_edge) / total_mass
    )
    second_lap = (
        assemble(node_mass * laplace(first_lap, geometry), True, nbr_face, nbr_edge) / total_mass
    )
    return sectioned - hyper_coeff * second_lap


SIDE = 8
HALF = 64


def tile_place(edge, kind, block, last):
    if kind == 0:
        return jnp.where(edge == 0, 0, last), jnp.where(edge == 0, block, last - block)
    return jnp.where(edge == 1, block, last - block), jnp.where(edge == 1, last, 0)


def kernel(
    groups,
    blocks,
    nbr_face,
    nbr_edge,
    state,
    jac,
    diag,
    cross,
    coriolis,
    out,
    *scratch,
):
    faces = state.shape[0]
    pairs = (faces + 1) // 2
    planes = faces + pairs
    fields, cols, packs, got_col, got_row, got_pack, rim_0, rim_1, end_0, end_1 = (
        scratch[i * ROUNDS : (i + 1) * ROUNDS] for i in range(10)
    )
    got_rim = [pair for pair in zip(rim_0, rim_1)]
    got_end = [pair for pair in zip(end_0, end_1)]
    summed, sectioned, inverse, flux_a, flux_b, flux_c = scratch[10 * ROUNDS : 10 * ROUNDS + 6]
    sem_s_near, sem_r_near, sem_s_rim, sem_r_rim, sem_s_end, sem_r_end = scratch[10 * ROUNDS + 6 :]
    g = lax.axis_index("face")
    y = lax.axis_index("fy")
    x = lax.axis_index("fx")
    last = blocks - 1

    barrier = pltpu.get_barrier_semaphore()
    for tg in range(groups):
        for ty in range(blocks):
            for tx in range(blocks):

                @pl.when(jnp.logical_not((g == tg) & (y == ty) & (x == tx)))
                def _():
                    pl.semaphore_signal(barrier, inc=1, device_id=(tg, ty, tx), device_id_type=MESH)

    live = ((y == 0) | (y == last), (x == 0) | (x == last))
    edge = (jnp.where(y == 0, 0, 2), jnp.where(x == 0, 3, 1))
    place = (jnp.where(y == 0, x, last - x), jnp.where(x == 0, last - y, y))
    at_end = (jnp.where(y == 0, 0, SIDE - 1), jnp.where(x == 0, 0, SIDE - 1))
    side = (jnp.where(y == 0, 0, 1), jnp.where(x == 0, 0, 1))
    head_pack = (jnp.where(y == 0, 0, 3), jnp.where(x == 0, 2, 1))
    tail_pack = (jnp.where(y == 0, 1, 2), jnp.where(x == 0, 0, 3))

    near = [(0, -1), (0, 1), (-1, 0), (1, 0), (-1, -1), (-1, 1), (1, -1), (1, 1)]

    def has(dy, dx):
        ok = None
        for d, at in ((dy, y), (dx, x)):
            if d:
                one = at > 0 if d < 0 else at < last
                ok = one if ok is None else ok & one
        return ok

    def near_slot(rnd, n):
        dy, dx = near[n]
        if dy == 0:
            return got_col[rnd].at[(dx + 1) // 2]
        if dx == 0:
            return got_row[rnd].at[(dy + 1) // 2]
        return got_pack[rnd].at[(dy + 1) + (dx + 1) // 2]

    def near_copy(rnd, n):
        dy, dx = near[n]
        back = near.index((-dy, -dx))
        if dy == 0:
            src = cols[rnd].at[(dx + 1) // 2]
        elif dx == 0:
            src = fields[rnd].at[:, (dy + 1) // 2 * (SIDE - 1)]
        else:
            src = packs[rnd].at[(dy + 1) + (dx + 1) // 2]
        return pltpu.make_async_remote_copy(
            src_ref=src,
            dst_ref=near_slot(rnd, back),
            send_sem=sem_s_near.at[n],
            recv_sem=sem_r_near.at[rnd, back],
            device_id=(g, y + dy, x + dx),
            device_id_type=MESH,
        )

    def near_wait(rnd, n):
        dy, dx = near[n]
        pltpu.make_async_remote_copy(
            src_ref=near_slot(rnd, n),
            dst_ref=near_slot(rnd, n),
            send_sem=sem_s_near.at[n],
            recv_sem=sem_r_near.at[rnd, n],
            device_id=(g, y + dy, x + dx),
            device_id_type=MESH,
        ).wait_recv()

    def each_rim(kind, which, visit):
        block = last - place[kind] + (0, 1, -1)[which]

        @pl.when(live[kind] & (block >= 0) & (block <= last))
        def _():
            for de in range(4):
                e2, kind2 = lax.rem(edge[kind] + de, 4), (kind + de) % 2
                ty, tx = tile_place(e2, kind2, block, last)
                for dg in range(groups):
                    g2 = lax.rem(g + dg, groups)
                    own = dg == 0 and (de in (1, 3) if which == 0 else de == 0)
                    visit(de, dg, e2, kind2, g2, (g2, ty, tx), (y == ty) & (x == tx) if own else None)

    def sides(mine, here, there):
        if mine is None:
            there()
            return
        pl.when(jnp.logical_not(mine))(there)
        if here is not None:
            pl.when(mine)(here)

    def rim_source(rnd, kind, which):
        if which == 0:
            return fields[rnd].at[:, at_end[0]] if kind == 0 else cols[rnd].at[side[1]]
        return packs[rnd].at[head_pack[kind] if which == 1 else tail_pack[kind]]

    def rim_slot(rnd, kind, which, e2, g2):
        if which == 0:
            return got_rim[rnd][kind].at[e2, g2], sem_r_rim.at[rnd, kind, e2, g2]
        return got_end[rnd][kind].at[which - 1, e2, g2], sem_r_end.at[rnd, kind, which - 1, e2, g2]

    def rim_sent(kind, which, de, dg):
        return sem_s_rim.at[kind, de, dg] if which == 0 else sem_s_end.at[kind, which - 1, de, dg]

    def rim_send(rnd, kind, which):
        src = rim_source(rnd, kind, which)

        def visit(de, dg, e2, kind2, g2, target, mine):
            dst, recv = rim_slot(rnd, kind2, which, edge[kind], g)

            def there():
                pltpu.make_async_remote_copy(
                    src_ref=src,
                    dst_ref=dst,
                    send_sem=rim_sent(kind, which, de, dg),
                    recv_sem=recv,
                    device_id=target,
                    device_id_type=MESH,
                ).start()

            def here():
                dst[...] = src[...]

            sides(mine, here, there)

        each_rim(kind, which, visit)

    def rim_wait_send(rnd, kind, which):
        src = rim_source(rnd, kind, which)

        def visit(de, dg, e2, kind2, g2, target, mine):
            dst, recv = rim_slot(rnd, kind2, which, edge[kind], g)

            def there():
                pltpu.make_async_remote_copy(
                    src_ref=src,
                    dst_ref=dst,
                    send_sem=rim_sent(kind, which, de, dg),
                    recv_sem=recv,
                    device_id=target,
                    device_id_type=MESH,
                ).wait_send()

            sides(mine, None, there)

        each_rim(kind, which, visit)

    def rim_wait(rnd, kind, which):
        def visit(de, dg, e2, kind2, g2, source, mine):
            dst, recv = rim_slot(rnd, kind, which, e2, g2)

            def there():
                pltpu.make_async_remote_copy(
                    src_ref=dst,
                    dst_ref=dst,
                    send_sem=rim_sent(kind, which, de, dg),
                    recv_sem=recv,
                    device_id=source,
                    device_id_type=MESH,
                ).wait_recv()

            sides(mine, None, there)

        each_rim(kind, which, visit)

    sub = lax.broadcasted_iota(jnp.int32, (SIDE, 128), 0)
    lane = lax.broadcasted_iota(jnp.int32, (SIDE, 128), 1)
    low = lane < HALF
    node = sub % 4
    table = deriv_table()
    weights = (1.0 / 6.0, 5.0 / 6.0, 5.0 / 6.0, 1.0 / 6.0)
    zero = jnp.zeros((SIDE, 128), jnp.float32)

    def per_node(entries):
        total = jnp.full((SIDE, 128), entries[0], jnp.float32)
        for j in range(1, 4):
            total = jnp.where(node == j, jnp.float32(entries[j]), total)
        return total

    col_weight = per_node(weights)
    taps = {
        s: per_node([float(table[j, j + s]) if 0 <= j + s < 4 else 0.0 for j in range(4)])
        for s in range(-3, 4)
    }

    def roll_rows(v, shift):
        return pltpu.roll(v, (-shift) % SIDE, 0)

    def swap(v):
        return pltpu.roll(v, HALF, 1)

    def dx(v):
        total = taps[0] * v
        for s in (-3, -2, -1, 1, 2, 3):
            total = total + taps[s] * roll_rows(v, s)
        return total

    def dy(rows):
        return [sum(jnp.float32(table[i, k]) * rows[k] for k in range(4)) for i in range(4)]

    def join(v):
        return v + jnp.where(sub == 3, roll_rows(v, 1), jnp.where(sub == 4, roll_rows(v, -1), zero))

    def wide(ref, index, r):
        row = jnp.broadcast_to(ref[index + (pl.ds(r, 1), slice(None))].reshape(1, SIDE), (SIDE, SIDE))
        eye = lax.broadcasted_iota(jnp.int32, (SIDE, SIDE), 0) == lax.broadcasted_iota(jnp.int32, (SIDE, SIDE), 1)
        return jnp.broadcast_to(jnp.sum(jnp.where(eye, row, 0.0), axis=1, keepdims=True), (SIDE, 128))

    def mass_mix(values):
        total = values[0]
        for f in range(1, faces):
            total = jnp.where(lane >= HALF + 16 * f, values[f], total)
        return total

    def pair_up(values, spare):
        return [
            jnp.where(low, values[2 * i], values[2 * i + 1] if 2 * i + 1 < faces else spare)
            for i in range(pairs)
        ]

    def store_field(rnd, plane, rows):
        rows = [join(v) for v in rows]
        for r in range(4, SIDE, 4):
            both = rows[r - 1] + rows[r]
            rows[r - 1] = both
            rows[r] = both
        for r, v in enumerate(rows):
            fields[rnd][plane, r] = v
            cols[rnd][0, plane, pl.ds(r, 1)] = v[0:1]
            cols[rnd][1, plane, pl.ds(r, 1)] = v[SIDE - 1 : SIDE]
        for w in range(4):
            v = rows[(SIDE - 1) * (w // 2)]
            c = (SIDE - 1) * (w % 2)
            packs[rnd][w, pl.ds(plane, 1)] = v[c : c + 1]

    def mirror(v):
        v = jnp.where(sub % 2 == 0, roll_rows(v, 1), roll_rows(v, -1))
        v = jnp.where(sub % 4 < 2, roll_rows(v, 2), roll_rows(v, -2))
        return pltpu.roll(v, 4, 0)

    def exchange(rnd):
        for n, (dy_, dx_) in enumerate(near):
            pl.when(has(dy_, dx_))(lambda n=n: near_copy(rnd, n).start())
        for which in range(3):
            for kind in range(2):
                rim_send(rnd, kind, which)

        for n, (dy_, dx_) in enumerate(near):
            ok = has(dy_, dx_)
            ref = near_slot(rnd, n)
            pl.when(ok)(lambda n=n: near_wait(rnd, n))

            @pl.when(jnp.logical_not(ok))
            def _():
                ref[...] = jnp.zeros(ref.shape, jnp.float32)

        def wide_row(ref, *index):
            return jnp.broadcast_to(ref[index], (SIDE, 128))

        for plane in range(planes):
            for r in range(SIDE):
                v = fields[rnd][plane, r]
                west = wide_row(got_col[rnd], 0, plane, pl.ds(r, 1))
                east = wide_row(got_col[rnd], 1, plane, pl.ds(r, 1))
                if r in (0, SIDE - 1):
                    w = 0 if r == 0 else 1
                    v = v + got_row[rnd][w, plane]
                    west = west + wide_row(got_pack[rnd], 2 * w, pl.ds(plane, 1))
                    east = east + wide_row(got_pack[rnd], 2 * w + 1, pl.ds(plane, 1))
                summed[plane, r] = v + jnp.where(sub == 0, west, jnp.where(sub == SIDE - 1, east, zero))

        for kind in range(2):
            for which in range(3):
                rim_wait(rnd, kind, which)

            @pl.when(live[kind] & (place[kind] == 0))
            def _():
                got_end[rnd][kind][0] = jnp.zeros(got_end[rnd][kind].shape[1:], jnp.float32)

            @pl.when(live[kind] & (place[kind] == last))
            def _():
                got_end[rnd][kind][1] = jnp.zeros(got_end[rnd][kind].shape[1:], jnp.float32)

            @pl.when(live[kind])
            def _():
                first_at = jnp.where(edge[kind] >= 2, SIDE - 1, 0)
                winds, temps, masses = [], [], []
                for f in range(faces):
                    nf = nbr_face[edge[kind], g * faces + f]
                    ne = nbr_edge[edge[kind], g * faces + f]
                    ng, nl = nf // faces, nf % faces
                    quarter = (edge[kind] - ne + 2) % 4
                    cosine = jnp.where(quarter == 0, 1.0, jnp.where(quarter == 2, -1.0, 0.0))
                    sine = jnp.where(quarter == 1, 1.0, jnp.where(quarter == 3, -1.0, 0.0))
                    sine = jnp.where(low, -sine, sine)
                    turned = (1 + jnp.where(edge[kind] >= 2, 1, 0) + jnp.where(ne >= 2, 1, 0)) % 2

                    def partner(plane):
                        v = got_rim[rnd][kind][ne, ng, plane]
                        v = jnp.where(turned == 1, mirror(v), v)
                        head = wide_row(got_end[rnd][kind], 0, ne, ng, pl.ds(plane, 1))
                        tail = wide_row(got_end[rnd][kind], 1, ne, ng, pl.ds(plane, 1))
                        return v + jnp.where(
                            sub == first_at, head, jnp.where(sub == SIDE - 1 - first_at, tail, zero)
                        )

                    v = partner(nl)
                    winds.append(cosine * v + sine * swap(v))
                    v = partner(faces + nl // 2)
                    temps.append(jnp.where(nl % 2 == f % 2, v, swap(v)))
                    if rnd == 0:
                        v = partner(planes - 1)
                        own = v
                        for k in range(faces):
                            if k != f:
                                own = jnp.where(nl == k, pltpu.roll(v, 16 * (f - k) % 128, 1), own)
                        masses.append(own)
                adds = winds + pair_up(temps, mass_mix(masses) if rnd == 0 else zero)
                for plane, rim in enumerate(adds):
                    if kind == 0:
                        summed[plane, at_end[0]] += rim
                    else:
                        for r in range(SIDE):
                            summed[plane, r] += jnp.where(
                                sub == at_end[1], jnp.broadcast_to(rim[r : r + 1], (SIDE, 128)), zero
                            )

        for n, (dy_, dx_) in enumerate(near):
            pl.when(has(dy_, dx_))(lambda n=n: near_copy(rnd, n).wait_send())
        for which in range(3):
            for kind in range(2):
                rim_wait_send(rnd, kind, which)

    section = [[None] * SIDE for _ in range(faces)]
    heat = [[None] * SIDE for _ in range(faces)]
    weight = [[None] * SIDE for _ in range(faces)]
    for f in range(faces):
        for start in range(0, SIDE, 4):
            wind, temp, contra, energy, vol, cor = [], [], [], [], [], []
            for r in range(start, start + 4):
                j = wide(jac, (f,), r)
                m_xx, m_yy, m_xy = wide(diag, (0, f), r), wide(diag, (1, f), r), wide(cross, (f,), r)
                flux_a[f, r] = j * m_xx
                flux_b[f, r] = j * m_xy
                flux_c[f, r] = j * m_yy
                w = state[f, r, :, 0 : 2 * HALF]
                t = state[f, r, :, 2 * HALF : 3 * HALF]
                t = jnp.concatenate([t, t], axis=1)
                c = jnp.where(low, m_xx, m_yy) * w + m_xy * swap(w)
                p = w * c
                wind.append(w)
                temp.append(t)
                contra.append(c)
                energy.append(0.5 * (p + swap(p)) + t)
                vol.append(j)
                cor.append(wide(coriolis, (f,), r))
                weight[f][r] = j * (jnp.float32(weights[r % 4]) * col_weight)
            dxs = [dx(jnp.where(low, energy[i], wind[i])) for i in range(4)]
            dys = dy([jnp.where(low, wind[i], energy[i]) for i in range(4)])
            dxt = [dx(temp[i]) for i in range(4)]
            dyt = dy(temp)
            for i in range(4):
                r = start + i
                dxv = jnp.where(low, swap(dxs[i]), dxs[i])
                dyu = jnp.where(low, dys[i], swap(dys[i]))
                spin = (dxv - dyu) + cor[i] * vol[i]
                spin = jnp.where(low, spin, -spin)
                tend = spin * swap(contra[i]) - jnp.where(low, dxs[i], dys[i])
                section[f][r] = weight[f][r] * (wind[i] + time_step * tend)
                q = contra[i] * jnp.where(low, dxt[i], dyt[i])
                heat[f][r] = weight[f][r] * (temp[i] - time_step * (q + swap(q)))
        store_field(0, f, section[f])
    mixed = [
        pair_up([heat[f][r] for f in range(faces)], mass_mix([weight[f][r] for f in range(faces)]))
        for r in range(SIDE)
    ]
    for i in range(pairs):
        store_field(0, faces + i, [mixed[r][i] for r in range(SIDE)])

    pl.semaphore_wait(barrier, groups * blocks * blocks - 1)
    exchange(0)

    def laplacian(rnd, source):
        for plane in range(planes):
            rows = []
            for start in range(0, SIDE, 4):
                at = range(start, start + 4)
                values = [source(plane, r) for r in at]
                coefs = [[ref[plane, r] for ref in (flux_a, flux_b, flux_c)] for r in at]
                gx = [dx(v) for v in values]
                gy = dy(values)
                fx = [c[0] * p + c[1] * q for c, p, q in zip(coefs, gx, gy)]
                fy = dy([c[1] * p + c[2] * q for c, p, q in zip(coefs, gx, gy)])
                rows += [(jnp.float32(weights[i]) * col_weight) * (dx(fx[i]) + fy[i]) for i in range(4)]
            store_field(rnd, plane, rows)

    for r in range(SIDE):
        spare = summed[planes - 1, r]
        inv = []
        for f in range(faces):
            at = HALF + 16 * f
            inv.append(1.0 / jnp.broadcast_to(spare[:, at : at + 1], (SIDE, 128)))
        for plane, v in enumerate(inv + pair_up(inv, inv[-1])):
            inverse[plane, r] = v
            sectioned[plane, r] = summed[plane, r] * v
        for ref in (flux_a, flux_b, flux_c):
            mine = [ref[f, r] for f in range(faces)]
            for i, v in enumerate(pair_up(mine, mine[-1])):
                ref[faces + i, r] = v
    laplacian(1, lambda plane, r: sectioned[plane, r])
    exchange(1)
    laplacian(2, lambda plane, r: summed[plane, r] * inverse[plane, r])
    exchange(2)
    for r in range(SIDE):
        done = [
            sectioned[plane, r] - hyper_coeff * (summed[plane, r] * inverse[plane, r]) for plane in range(planes)
        ]
        for f in range(faces):
            out[f, r, :, 0 : 2 * HALF] = done[f]
            t = done[faces + f // 2]
            out[f, r, :, 2 * HALF : 3 * HALF] = (t if f % 2 == 0 else swap(t))[:, 0:HALF]


def fused(groups, blocks, state, jacobian, metric_diag, metric_cross, coriolis, nbr_face, nbr_edge):
    faces = state.shape[0]
    planes = faces + (faces + 1) // 2
    piece = (planes, SIDE, 128)
    tile = (planes, SIDE, SIDE, 128)

    def per_round(shape):
        return [pltpu.VMEM(shape, jnp.float32)] * ROUNDS

    scratch = (
        per_round(tile)
        + per_round((2,) + piece)
        + per_round((4, planes, 128))
        + per_round((2,) + piece)
        + per_round((2,) + piece)
        + per_round((4, planes, 128))
        + per_round((4, groups) + piece) * 2
        + per_round((2, 4, groups, planes, 128)) * 2
        + [pltpu.VMEM(tile, jnp.float32)] * 6
        + [
            pltpu.SemaphoreType.DMA((8,)),
            pltpu.SemaphoreType.DMA((ROUNDS, 8)),
            pltpu.SemaphoreType.DMA((2, 4, groups)),
            pltpu.SemaphoreType.DMA((ROUNDS, 2, 4, groups)),
            pltpu.SemaphoreType.DMA((2, 2, 4, groups)),
            pltpu.SemaphoreType.DMA((ROUNDS, 2, 2, 4, groups)),
        ]
    )
    vmem, smem = pl.BlockSpec(memory_space=pltpu.VMEM), pl.BlockSpec(memory_space=pltpu.SMEM)
    return pl.pallas_call(
        functools.partial(kernel, groups, blocks),
        out_shape=jax.ShapeDtypeStruct(state.shape, jnp.float32),
        in_specs=[smem, smem] + [vmem] * 5,
        out_specs=vmem,
        scratch_shapes=scratch,
        compiler_params=pltpu.CompilerParams(collective_id=0, has_side_effects=True),
    )(nbr_face.T, nbr_edge.T, state, jacobian, metric_diag, metric_cross, coriolis)


def solution(mesh):
    groups, rows, columns = (mesh.shape[axis] for axis in ("face", "fy", "fx"))

    def body(*args):
        state = args[0]
        faces = state.shape[0]
        if rows == columns and rows > 1 and state.shape[1:] == (SIDE, SIDE, 3 * HALF) and faces in (1, 3):
            return fused(groups, rows, *args)
        return per_device(*args)

    return jax.shard_map(
        body,
        mesh=mesh,
        in_specs=(
            P("face", "fy", "fx", None),
            P("face", "fy", "fx"),
            P(None, "face", "fy", "fx"),
            P("face", "fy", "fx"),
            P("face", "fy", "fx"),
            P(),
            P(),
        ),
        out_specs=P("face", "fy", "fx", None),
        check_vma=False,
    )
```

```python
import functools

import jax
import jax.numpy as jnp
import numpy as np
from jax import lax
from jax.experimental import pallas as pl
from jax.experimental.pallas import tpu as pltpu
from jax.sharding import PartitionSpec as P

time_step = 0.05
hyper_coeff = 0.0005
MESH = pl.DeviceIdType.MESH
ROUNDS = 3


def padded(cells, sides, width):
    for axis, dim in sides:
        count = lax.axis_size(axis)
        ends = count - 1
        head = lax.slice_in_dim(cells, 0, width, axis=dim)
        tail = lax.slice_in_dim(cells, cells.shape[dim] - width, cells.shape[dim], axis=dim)
        cells = jnp.concatenate(
            [
                lax.ppermute(tail, axis, [(i, (i + 1) % count) for i in range(ends)]),
                cells,
                lax.ppermute(head, axis, [((i + 1) % count, i) for i in range(ends)]),
            ],
            axis=dim,
        )
    return cells


def deriv_table():
    gll_nodes = np.array([-1.0, -1.0 / np.sqrt(5.0), 1.0 / np.sqrt(5.0), 1.0])
    bary_weights = np.ones(4)
    for j in range(4):
        for m in range(4):
            if m != j:
                bary_weights[j] = bary_weights[j] / (gll_nodes[j] - gll_nodes[m])
    matrix = np.zeros((4, 4))
    for i in range(4):
        for j in range(4):
            if i != j:
                matrix[i, j] = bary_weights[j] / bary_weights[i] / (gll_nodes[i] - gll_nodes[j])
        matrix[i, i] = -np.sum(matrix[i])
    return matrix


def along_x(values):
    face_count, row_count, col_count, chan_count = values.shape
    blocks = values.reshape(face_count, row_count, col_count // 4, 4, chan_count)
    result = jnp.einsum(
        "jk,abekc->abejc",
        jnp.asarray(deriv_table(), jnp.float32),
        blocks,
        precision=lax.Precision.HIGHEST,
    )
    return result.reshape(values.shape)


def along_y(values):
    face_count, row_count, col_count, chan_count = values.shape
    blocks = values.reshape(face_count, row_count // 4, 4, col_count, chan_count)
    result = jnp.einsum(
        "ik,aekxc->aeixc",
        jnp.asarray(deriv_table(), jnp.float32),
        blocks,
        precision=lax.Precision.HIGHEST,
    )
    return result.reshape(values.shape)


def mass_of(jacobian):
    weights = jnp.asarray([1.0 / 6.0, 5.0 / 6.0, 5.0 / 6.0, 1.0 / 6.0], jnp.float32)
    row_weight = jnp.tile(weights, jacobian.shape[1] // 4)
    col_weight = jnp.tile(weights, jacobian.shape[2] // 4)
    return jacobian * row_weight[None, :, None] * col_weight[None, None, :]


def tendency(state, geometry, planet):
    volume, metric_xx, metric_yy, metric_xy = geometry
    levels = state.shape[-1] // 3
    wind_u = state[..., :levels]
    wind_v = state[..., levels : 2 * levels]
    temper = state[..., 2 * levels :]
    contra_u = metric_xx * wind_u + metric_xy * wind_v
    contra_v = metric_xy * wind_u + metric_yy * wind_v
    energy = 0.5 * (wind_u * contra_u + wind_v * contra_v) + temper
    xderivs = along_x(jnp.concatenate([wind_v, temper, energy], -1))
    yderivs = along_y(jnp.concatenate([wind_u, temper, energy], -1))
    absolute = (xderivs[..., :levels] - yderivs[..., :levels]) / volume + planet
    tend_u = absolute * volume * contra_v - xderivs[..., 2 * levels :]
    tend_v = -absolute * volume * contra_u - yderivs[..., 2 * levels :]
    tend_t = -(
        contra_u * xderivs[..., levels : 2 * levels] + contra_v * yderivs[..., levels : 2 * levels]
    )
    return state + time_step * jnp.concatenate([tend_u, tend_v, tend_t], -1)


def laplace(values, geometry):
    volume, metric_xx, metric_yy, metric_xy = geometry
    grad_x = along_x(values)
    grad_y = along_y(values)
    flux_x = volume * (metric_xx * grad_x + metric_xy * grad_y)
    flux_y = volume * (metric_xy * grad_x + metric_yy * grad_y)
    return (along_x(flux_x) + along_y(flux_y)) / volume


def combine(values, axis):
    length = values.shape[axis] - 2
    positions = jnp.arange(length)
    leading = (positions % 4 == 0).astype(jnp.float32)
    trailing = (positions % 4 == 3).astype(jnp.float32)
    broad_shape = [1, 1, 1, 1]
    broad_shape[axis] = length
    leading = leading.reshape(broad_shape)
    trailing = trailing.reshape(broad_shape)
    middle = lax.slice_in_dim(values, 1, length + 1, axis=axis)
    previous = lax.slice_in_dim(values, 0, length, axis=axis)
    following = lax.slice_in_dim(values, 2, length + 2, axis=axis)
    return middle + leading * previous + trailing * following


def rotate(segment, quarter, levels):
    cosine = ((quarter == 0).astype(jnp.float32) - (quarter == 2).astype(jnp.float32))[..., None]
    sine_part = ((quarter == 1).astype(jnp.float32) - (quarter == 3).astype(jnp.float32))[..., None]
    wind_u = segment[..., :levels]
    wind_v = segment[..., levels : 2 * levels]
    return jnp.concatenate(
        [
            cosine * wind_u - sine_part * wind_v,
            sine_part * wind_u + cosine * wind_v,
            segment[..., 2 * levels :],
        ],
        -1,
    )


def in_face(values):
    across = combine(padded(values, (("fx", 2),), 1), 2)
    return combine(padded(across, (("fy", 1),), 1), 1)


def place_pieces(
    got_flat,
    got_tall,
    vector,
    nbr_edge,
    flat_edge,
    tall_edge,
    on_south,
    on_west,
    flat_start,
    tall_start,
    face_local,
    side_nodes,
    chan_count,
    levels,
):
    edge_ids = jnp.arange(4, dtype=jnp.int32)
    flat_target = nbr_edge[:, flat_edge]
    tall_target = nbr_edge[:, tall_edge]
    if vector:
        got_flat = rotate(got_flat, ((flat_target - flat_edge + 2) % 4)[None, :, None], levels)
        got_tall = rotate(got_tall, ((tall_target - tall_edge + 2) % 4)[None, :, None], levels)
    got_flat = jnp.where(on_south, got_flat[:, :, ::-1], got_flat)
    got_tall = jnp.where(on_west, got_tall, got_tall[:, :, ::-1])
    flat_pick = (flat_target[:, None] == edge_ids[None, :]).astype(jnp.float32)
    tall_pick = (tall_target[:, None] == edge_ids[None, :]).astype(jnp.float32)
    flat_rims = jnp.einsum("se,gsjc->gejc", flat_pick, got_flat, precision=lax.Precision.HIGHEST)
    tall_rims = jnp.einsum("se,gsjc->gejc", tall_pick, got_tall, precision=lax.Precision.HIGHEST)
    empty_rims = jnp.zeros((face_local, 4, side_nodes, chan_count), jnp.float32)
    rim_strips = lax.dynamic_update_slice(empty_rims, flat_rims, (0, 0, flat_start, 0))
    return rim_strips + lax.dynamic_update_slice(empty_rims, tall_rims, (0, 0, tall_start, 0))


def outgoing(
    summed, nbr_face, face_ids, flat_edge, tall_edge, on_south, on_west, flat_live, tall_live
):
    row_count = summed.shape[1]
    col_count = summed.shape[2]
    all_faces = jnp.arange(nbr_face.shape[0], dtype=jnp.int32)
    flat_piece = jnp.where(on_south, summed[:, 0], summed[:, row_count - 1])
    tall_piece = jnp.where(on_west, summed[:, :, 0], summed[:, :, col_count - 1])
    flat_dest = nbr_face[face_ids, flat_edge]
    tall_dest = nbr_face[face_ids, tall_edge]
    flat_send = ((all_faces[:, None] == flat_dest[None, :]) & flat_live).astype(jnp.float32)
    tall_send = ((all_faces[:, None] == tall_dest[None, :]) & tall_live).astype(jnp.float32)
    return (
        flat_send[:, :, None, None] * flat_piece[None],
        tall_send[:, :, None, None] * tall_piece[None],
    )


def assemble(values, vector, nbr_face, nbr_edge):
    summed = in_face(values)
    face_local, row_count, col_count, chan_count = summed.shape
    levels = chan_count // 3
    row_index = lax.axis_index("fy")
    col_index = lax.axis_index("fx")
    side_nodes = row_count * lax.axis_size("fy")
    face_ids = lax.axis_index("face") * face_local + jnp.arange(face_local, dtype=jnp.int32)
    on_south = row_index == 0
    on_north = row_index == lax.axis_size("fy") - 1
    on_west = col_index == 0
    on_east = col_index == lax.axis_size("fx") - 1
    flat_live = on_south | on_north
    tall_live = on_west | on_east
    flat_edge = jnp.where(on_south, 0, 2).astype(jnp.int32)
    tall_edge = jnp.where(on_west, 3, 1).astype(jnp.int32)
    flat_start = jnp.where(
        on_south, side_nodes - (col_index + 1) * col_count, col_index * col_count
    )
    tall_start = jnp.where(on_west, row_index * row_count, side_nodes - (row_index + 1) * row_count)
    send_flat, send_tall = outgoing(
        summed, nbr_face, face_ids, flat_edge, tall_edge, on_south, on_west, flat_live, tall_live
    )
    got_flat, got_tall = (
        lax.all_to_all(send_flat, "face", split_axis=0, concat_axis=1, tiled=True),
        lax.all_to_all(send_tall, "face", split_axis=0, concat_axis=1, tiled=True),
    )
    rim_strips = place_pieces(
        got_flat,
        got_tall,
        vector,
        nbr_edge,
        flat_edge,
        tall_edge,
        on_south,
        on_west,
        flat_start,
        tall_start,
        face_local,
        side_nodes,
        chan_count,
        levels,
    )
    flat_lines = jnp.stack([rim_strips[:, 0], rim_strips[:, 2, ::-1]], axis=1)
    flat_lines = flat_lines.reshape(face_local, 2, lax.axis_size("fx"), col_count, chan_count)
    tall_lines = jnp.stack([rim_strips[:, 1], rim_strips[:, 3, ::-1]], axis=1)
    tall_lines = tall_lines.reshape(face_local, 2, lax.axis_size("fy"), row_count, chan_count)
    flat_whole = lax.psum(flat_lines, "fy")
    tall_whole = lax.psum(tall_lines, "fx")
    flat_block = lax.psum_scatter(flat_whole, "fx", scatter_dimension=2, tiled=True)
    tall_block = lax.psum_scatter(tall_whole, "fy", scatter_dimension=2, tiled=True)
    flat_add = jnp.where(on_south, flat_block[:, 0, 0], flat_block[:, 1, 0])
    tall_add = jnp.where(on_west, tall_block[:, 1, 0], tall_block[:, 0, 0])
    result = summed.at[:, 0].add(jnp.where(on_south, flat_add, 0.0))
    result = result.at[:, row_count - 1].add(jnp.where(on_north, flat_add, 0.0))
    result = result.at[:, :, 0].add(jnp.where(on_west, tall_add, 0.0))
    result = result.at[:, :, col_count - 1].add(jnp.where(on_east, tall_add, 0.0))
    return result


def per_device(state, jacobian, metric_diag, metric_cross, coriolis, nbr_face, nbr_edge):
    node_mass = mass_of(jacobian)[..., None]
    total_mass = assemble(node_mass, False, nbr_face, nbr_edge)
    geometry = (
        jacobian[..., None],
        metric_diag[0][..., None],
        metric_diag[1][..., None],
        metric_cross[..., None],
    )
    raw = tendency(state, geometry, coriolis[..., None])
    sectioned = assemble(node_mass * raw, True, nbr_face, nbr_edge) / total_mass
    first_lap = (
        assemble(node_mass * laplace(sectioned, geometry), True, nbr_face, nbr_edge) / total_mass
    )
    second_lap = (
        assemble(node_mass * laplace(first_lap, geometry), True, nbr_face, nbr_edge) / total_mass
    )
    return sectioned - hyper_coeff * second_lap


SIDE = 8
HALF = 64


def tile_place(edge, kind, block, last):
    if kind == 0:
        return jnp.where(edge == 0, 0, last), jnp.where(edge == 0, block, last - block)
    return jnp.where(edge == 1, block, last - block), jnp.where(edge == 1, last, 0)


def kernel(
    groups,
    blocks,
    nbr_face,
    nbr_edge,
    state,
    jac,
    diag,
    cross,
    coriolis,
    out,
    *scratch,
):
    faces = state.shape[0]
    pairs = (faces + 1) // 2
    planes = faces + pairs
    fields, cols, packs, got_col, got_row, got_pack, rim_0, rim_1, end_0, end_1 = (
        scratch[i * ROUNDS : (i + 1) * ROUNDS] for i in range(10)
    )
    got_rim = [pair for pair in zip(rim_0, rim_1)]
    got_end = [pair for pair in zip(end_0, end_1)]
    summed, sectioned, inverse, flux_a, flux_b, flux_c = scratch[10 * ROUNDS : 10 * ROUNDS + 6]
    sem_s_near, sem_r_near, sem_s_rim, sem_r_rim, sem_s_own, sem_r_own = scratch[10 * ROUNDS + 6 :]
    g = lax.axis_index("face")
    y = lax.axis_index("fy")
    x = lax.axis_index("fx")
    last = blocks - 1

    barrier = pltpu.get_barrier_semaphore()
    for tg in range(groups):
        for ty in range(blocks):
            for tx in range(blocks):

                @pl.when(jnp.logical_not((g == tg) & (y == ty) & (x == tx)))
                def _():
                    pl.semaphore_signal(barrier, inc=1, device_id=(tg, ty, tx), device_id_type=MESH)

    live = ((y == 0) | (y == last), (x == 0) | (x == last))
    edge = (jnp.where(y == 0, 0, 2), jnp.where(x == 0, 3, 1))
    place = (jnp.where(y == 0, x, last - x), jnp.where(x == 0, last - y, y))
    at_end = (jnp.where(y == 0, 0, SIDE - 1), jnp.where(x == 0, 0, SIDE - 1))
    side = (jnp.where(y == 0, 0, 1), jnp.where(x == 0, 0, 1))
    head_pack = (jnp.where(y == 0, 0, 3), jnp.where(x == 0, 2, 1))
    tail_pack = (jnp.where(y == 0, 1, 2), jnp.where(x == 0, 0, 3))

    near = [(0, -1), (0, 1), (-1, 0), (1, 0), (-1, -1), (-1, 1), (1, -1), (1, 1)]

    def has(dy, dx):
        ok = None
        for d, at in ((dy, y), (dx, x)):
            if d:
                one = at > 0 if d < 0 else at < last
                ok = one if ok is None else ok & one
        return ok

    def near_slot(rnd, n):
        dy, dx = near[n]
        if dy == 0:
            return got_col[rnd].at[(dx + 1) // 2]
        if dx == 0:
            return got_row[rnd].at[(dy + 1) // 2]
        return got_pack[rnd].at[(dy + 1) + (dx + 1) // 2]

    def near_copy(rnd, n):
        dy, dx = near[n]
        back = near.index((-dy, -dx))
        if dy == 0:
            src = cols[rnd].at[(dx + 1) // 2]
        elif dx == 0:
            src = fields[rnd].at[:, (dy + 1) // 2 * (SIDE - 1)]
        else:
            src = packs[rnd].at[(dy + 1) + (dx + 1) // 2]
        return pltpu.make_async_remote_copy(
            src_ref=src,
            dst_ref=near_slot(rnd, back),
            send_sem=sem_s_near.at[n],
            recv_sem=sem_r_near.at[rnd, back],
            device_id=(g, y + dy, x + dx),
            device_id_type=MESH,
        )

    def near_wait(rnd, n):
        dy, dx = near[n]
        pltpu.make_async_remote_copy(
            src_ref=near_slot(rnd, n),
            dst_ref=near_slot(rnd, n),
            send_sem=sem_s_near.at[n],
            recv_sem=sem_r_near.at[rnd, n],
            device_id=(g, y + dy, x + dx),
            device_id_type=MESH,
        ).wait_recv()

    def each_rim(kind, which, visit):
        block = last - place[kind] + (0, 1, -1)[which]

        @pl.when(live[kind] & (block >= 0) & (block <= last))
        def _():
            for de in (2, 1, 3, 0):
                e2, kind2 = lax.rem(edge[kind] + de, 4), (kind + de) % 2
                ty, tx = tile_place(e2, kind2, block, last)
                for dg in range(groups):
                    g2 = lax.rem(g + dg, groups)
                    own = dg == 0 and (de in (1, 3) if which == 0 else de == 0)
                    visit(de, dg, e2, kind2, g2, (g2, ty, tx), (y == ty) & (x == tx) if own else None)

    def sides(mine, here, there):
        if mine is None:
            there()
            return
        pl.when(jnp.logical_not(mine))(there)
        if here is not None:
            pl.when(mine)(here)

    def rim_source(rnd, kind, which):
        if which == 0:
            return fields[rnd].at[:, at_end[0]] if kind == 0 else cols[rnd].at[side[1]]
        return packs[rnd].at[head_pack[kind] if which == 1 else tail_pack[kind]]

    def rim_slot(rnd, kind, which, e2, g2):
        at = e2 * groups + g2
        return got_rim[rnd][kind].at[at] if which == 0 else got_end[rnd][kind].at[which - 1, at]

    def rim_shared(rnd, kind, which):
        shared = pl.ds(0, 4 * groups - (2 if which == 0 else 1))
        return got_rim[rnd][kind].at[shared] if which == 0 else got_end[rnd][kind].at[which - 1, shared]

    def rim_sent(kind, which, de, dg):
        return pick(sem_s_rim.at[kind, which], sem_s_own.at[kind, which], which, de, dg)

    def rim_got(rnd, kind, which, de, dg):
        return pick(sem_r_rim.at[rnd, kind, which], sem_r_own.at[rnd, kind, which], which, de, dg)

    def pick(shared, own, which, de, dg):
        if dg or not (de in (1, 3) if which == 0 else de == 0):
            return shared
        return own.at[de // 2]

    def rim_copy(rnd, kind, which, src, dst, de, dg, kind2, back, device):
        return pltpu.make_async_remote_copy(
            src_ref=src,
            dst_ref=dst,
            send_sem=rim_sent(kind, which, de, dg),
            recv_sem=rim_got(rnd, kind2, which, back, dg),
            device_id=device,
            device_id_type=MESH,
        )

    def rim_send(rnd, kind, which):
        src = rim_source(rnd, kind, which)

        def visit(de, dg, e2, kind2, g2, target, mine):
            dst = rim_slot(rnd, kind2, which, edge[kind], g)

            def there():
                rim_copy(rnd, kind, which, src, dst, de, dg, kind2, (4 - de) % 4, target).start()

            def here():
                dst[...] = src[...]

            sides(mine, here, there)

        each_rim(kind, which, visit)

    def rim_waits(rnd, kind, which, received):
        first = []

        def visit(de, dg, e2, kind2, g2, device, mine):
            whole = mine is None
            if whole and first:
                return
            if whole:
                first.append(de)
            ref = rim_shared(rnd, kind, which) if whole else rim_slot(rnd, kind, which, e2, g2)

            def there():
                copy = rim_copy(rnd, kind, which, ref, ref, de, dg, kind, de, device)
                copy.wait_recv() if received else copy.wait_send()

            sides(mine, None, there)

        each_rim(kind, which, visit)

    def rim_wait(rnd, kind, which):
        rim_waits(rnd, kind, which, True)

    def rim_wait_send(rnd, kind, which):
        rim_waits(rnd, kind, which, False)

    sub = lax.broadcasted_iota(jnp.int32, (SIDE, 128), 0)
    lane = lax.broadcasted_iota(jnp.int32, (SIDE, 128), 1)
    low = lane < HALF
    node = sub % 4
    table = deriv_table()
    weights = (1.0 / 6.0, 5.0 / 6.0, 5.0 / 6.0, 1.0 / 6.0)
    zero = jnp.zeros((SIDE, 128), jnp.float32)

    def per_node(entries):
        total = jnp.full((SIDE, 128), entries[0], jnp.float32)
        for j in range(1, 4):
            total = jnp.where(node == j, jnp.float32(entries[j]), total)
        return total

    col_weight = per_node(weights)
    taps = {
        s: per_node([float(table[j, j + s]) if 0 <= j + s < 4 else 0.0 for j in range(4)])
        for s in range(-3, 4)
    }

    def roll_rows(v, shift):
        return pltpu.roll(v, (-shift) % SIDE, 0)

    def swap(v):
        return pltpu.roll(v, HALF, 1)

    def dx(v):
        total = taps[0] * v
        for s in (-3, -2, -1, 1, 2, 3):
            total = total + taps[s] * roll_rows(v, s)
        return total

    def dy(rows):
        return [sum(jnp.float32(table[i, k]) * rows[k] for k in range(4)) for i in range(4)]

    def join(v):
        return v + jnp.where(sub == 3, roll_rows(v, 1), jnp.where(sub == 4, roll_rows(v, -1), zero))

    def wide(ref, index, r):
        row = jnp.broadcast_to(ref[index + (pl.ds(r, 1), slice(None))].reshape(1, SIDE), (SIDE, SIDE))
        eye = lax.broadcasted_iota(jnp.int32, (SIDE, SIDE), 0) == lax.broadcasted_iota(jnp.int32, (SIDE, SIDE), 1)
        return jnp.broadcast_to(jnp.sum(jnp.where(eye, row, 0.0), axis=1, keepdims=True), (SIDE, 128))

    def mass_mix(values):
        total = values[0]
        for f in range(1, faces):
            total = jnp.where(lane >= HALF + 16 * f, values[f], total)
        return total

    def pair_up(values, spare):
        return [
            jnp.where(low, values[2 * i], values[2 * i + 1] if 2 * i + 1 < faces else spare)
            for i in range(pairs)
        ]

    def store_field(rnd, plane, rows):
        rows = [join(v) for v in rows]
        for r in range(4, SIDE, 4):
            both = rows[r - 1] + rows[r]
            rows[r - 1] = both
            rows[r] = both
        for r, v in enumerate(rows):
            fields[rnd][plane, r] = v
            cols[rnd][0, plane, pl.ds(r, 1)] = v[0:1]
            cols[rnd][1, plane, pl.ds(r, 1)] = v[SIDE - 1 : SIDE]
        for w in range(4):
            v = rows[(SIDE - 1) * (w // 2)]
            c = (SIDE - 1) * (w % 2)
            packs[rnd][w, pl.ds(plane, 1)] = v[c : c + 1]

    def mirror(v):
        v = jnp.where(sub % 2 == 0, roll_rows(v, 1), roll_rows(v, -1))
        v = jnp.where(sub % 4 < 2, roll_rows(v, 2), roll_rows(v, -2))
        return pltpu.roll(v, 4, 0)

    def exchange(rnd):
        for n, (dy_, dx_) in enumerate(near):
            pl.when(has(dy_, dx_))(lambda n=n: near_copy(rnd, n).start())
        for which in (1, 2, 0):
            for kind in range(2):
                rim_send(rnd, kind, which)

        for n, (dy_, dx_) in enumerate(near):
            ok = has(dy_, dx_)
            ref = near_slot(rnd, n)
            pl.when(ok)(lambda n=n: near_wait(rnd, n))

            @pl.when(jnp.logical_not(ok))
            def _():
                ref[...] = jnp.zeros(ref.shape, jnp.float32)

        def wide_row(ref, *index):
            return jnp.broadcast_to(ref[index], (SIDE, 128))

        for plane in range(planes):
            for r in range(SIDE):
                v = fields[rnd][plane, r]
                west = wide_row(got_col[rnd], 0, plane, pl.ds(r, 1))
                east = wide_row(got_col[rnd], 1, plane, pl.ds(r, 1))
                if r in (0, SIDE - 1):
                    w = 0 if r == 0 else 1
                    v = v + got_row[rnd][w, plane]
                    west = west + wide_row(got_pack[rnd], 2 * w, pl.ds(plane, 1))
                    east = east + wide_row(got_pack[rnd], 2 * w + 1, pl.ds(plane, 1))
                summed[plane, r] = v + jnp.where(sub == 0, west, jnp.where(sub == SIDE - 1, east, zero))

        for kind in range(2):
            for which in range(3):
                rim_wait(rnd, kind, which)

            @pl.when(live[kind] & (place[kind] == 0))
            def _():
                got_end[rnd][kind][0] = jnp.zeros(got_end[rnd][kind].shape[1:], jnp.float32)

            @pl.when(live[kind] & (place[kind] == last))
            def _():
                got_end[rnd][kind][1] = jnp.zeros(got_end[rnd][kind].shape[1:], jnp.float32)

            @pl.when(live[kind])
            def _():
                first_at = jnp.where(edge[kind] >= 2, SIDE - 1, 0)
                winds, temps, masses = [], [], []
                for f in range(faces):
                    nf = nbr_face[edge[kind], g * faces + f]
                    ne = nbr_edge[edge[kind], g * faces + f]
                    ng, nl = nf // faces, nf % faces
                    quarter = (edge[kind] - ne + 2) % 4
                    cosine = jnp.where(quarter == 0, 1.0, jnp.where(quarter == 2, -1.0, 0.0))
                    sine = jnp.where(quarter == 1, 1.0, jnp.where(quarter == 3, -1.0, 0.0))
                    sine = jnp.where(low, -sine, sine)
                    turned = (1 + jnp.where(edge[kind] >= 2, 1, 0) + jnp.where(ne >= 2, 1, 0)) % 2

                    def partner(plane):
                        v = got_rim[rnd][kind][ne * groups + ng, plane]
                        v = jnp.where(turned == 1, mirror(v), v)
                        head = wide_row(got_end[rnd][kind], 0, ne * groups + ng, pl.ds(plane, 1))
                        tail = wide_row(got_end[rnd][kind], 1, ne * groups + ng, pl.ds(plane, 1))
                        return v + jnp.where(
                            sub == first_at, head, jnp.where(sub == SIDE - 1 - first_at, tail, zero)
                        )

                    v = partner(nl)
                    winds.append(cosine * v + sine * swap(v))
                    v = partner(faces + nl // 2)
                    temps.append(jnp.where(nl % 2 == f % 2, v, swap(v)))
                    if rnd == 0:
                        v = partner(planes - 1)
                        own = v
                        for k in range(faces):
                            if k != f:
                                own = jnp.where(nl == k, pltpu.roll(v, 16 * (f - k) % 128, 1), own)
                        masses.append(own)
                adds = winds + pair_up(temps, mass_mix(masses) if rnd == 0 else zero)
                for plane, rim in enumerate(adds):
                    if kind == 0:
                        summed[plane, at_end[0]] += rim
                    else:
                        for r in range(SIDE):
                            summed[plane, r] += jnp.where(
                                sub == at_end[1], jnp.broadcast_to(rim[r : r + 1], (SIDE, 128)), zero
                            )

        for n, (dy_, dx_) in enumerate(near):
            pl.when(has(dy_, dx_))(lambda n=n: near_copy(rnd, n).wait_send())
        for which in range(3):
            for kind in range(2):
                rim_wait_send(rnd, kind, which)

    section = [[None] * SIDE for _ in range(faces)]
    heat = [[None] * SIDE for _ in range(faces)]
    weight = [[None] * SIDE for _ in range(faces)]
    for f in range(faces):
        for start in range(0, SIDE, 4):
            wind, temp, contra, energy, vol, cor = [], [], [], [], [], []
            for r in range(start, start + 4):
                j = wide(jac, (f,), r)
                m_xx, m_yy, m_xy = wide(diag, (0, f), r), wide(diag, (1, f), r), wide(cross, (f,), r)
                flux_a[f, r] = j * m_xx
                flux_b[f, r] = j * m_xy
                flux_c[f, r] = j * m_yy
                w = state[f, r, :, 0 : 2 * HALF]
                t = state[f, r, :, 2 * HALF : 3 * HALF]
                t = jnp.concatenate([t, t], axis=1)
                c = jnp.where(low, m_xx, m_yy) * w + m_xy * swap(w)
                p = w * c
                wind.append(w)
                temp.append(t)
                contra.append(c)
                energy.append(0.5 * (p + swap(p)) + t)
                vol.append(j)
                cor.append(wide(coriolis, (f,), r))
                weight[f][r] = j * (jnp.float32(weights[r % 4]) * col_weight)
            dxs = [dx(jnp.where(low, energy[i], wind[i])) for i in range(4)]
            dys = dy([jnp.where(low, wind[i], energy[i]) for i in range(4)])
            dxt = [dx(temp[i]) for i in range(4)]
            dyt = dy(temp)
            for i in range(4):
                r = start + i
                dxv = jnp.where(low, swap(dxs[i]), dxs[i])
                dyu = jnp.where(low, dys[i], swap(dys[i]))
                spin = (dxv - dyu) + cor[i] * vol[i]
                spin = jnp.where(low, spin, -spin)
                tend = spin * swap(contra[i]) - jnp.where(low, dxs[i], dys[i])
                section[f][r] = weight[f][r] * (wind[i] + time_step * tend)
                q = contra[i] * jnp.where(low, dxt[i], dyt[i])
                heat[f][r] = weight[f][r] * (temp[i] - time_step * (q + swap(q)))
        store_field(0, f, section[f])
    mixed = [
        pair_up([heat[f][r] for f in range(faces)], mass_mix([weight[f][r] for f in range(faces)]))
        for r in range(SIDE)
    ]
    for i in range(pairs):
        store_field(0, faces + i, [mixed[r][i] for r in range(SIDE)])

    pl.semaphore_wait(barrier, groups * blocks * blocks - 1)
    exchange(0)

    def laplacian(rnd, source):
        for plane in range(planes):
            rows = []
            for start in range(0, SIDE, 4):
                at = range(start, start + 4)
                values = [source(plane, r) for r in at]
                coefs = [[ref[plane, r] for ref in (flux_a, flux_b, flux_c)] for r in at]
                gx = [dx(v) for v in values]
                gy = dy(values)
                fx = [c[0] * p + c[1] * q for c, p, q in zip(coefs, gx, gy)]
                fy = dy([c[1] * p + c[2] * q for c, p, q in zip(coefs, gx, gy)])
                rows += [(jnp.float32(weights[i]) * col_weight) * (dx(fx[i]) + fy[i]) for i in range(4)]
            store_field(rnd, plane, rows)

    for r in range(SIDE):
        spare = summed[planes - 1, r]
        inv = []
        for f in range(faces):
            at = HALF + 16 * f
            inv.append(1.0 / jnp.broadcast_to(spare[:, at : at + 1], (SIDE, 128)))
        for plane, v in enumerate(inv + pair_up(inv, inv[-1])):
            inverse[plane, r] = v
            sectioned[plane, r] = summed[plane, r] * v
        for ref in (flux_a, flux_b, flux_c):
            mine = [ref[f, r] for f in range(faces)]
            for i, v in enumerate(pair_up(mine, mine[-1])):
                ref[faces + i, r] = v
    laplacian(1, lambda plane, r: sectioned[plane, r])
    exchange(1)
    laplacian(2, lambda plane, r: summed[plane, r] * inverse[plane, r])
    exchange(2)
    for r in range(SIDE):
        done = [
            sectioned[plane, r] - hyper_coeff * (summed[plane, r] * inverse[plane, r]) for plane in range(planes)
        ]
        for f in range(faces):
            out[f, r, :, 0 : 2 * HALF] = done[f]
            t = done[faces + f // 2]
            out[f, r, :, 2 * HALF : 3 * HALF] = (t if f % 2 == 0 else swap(t))[:, 0:HALF]


def fused(groups, blocks, state, jacobian, metric_diag, metric_cross, coriolis, nbr_face, nbr_edge):
    faces = state.shape[0]
    planes = faces + (faces + 1) // 2
    piece = (planes, SIDE, 128)
    tile = (planes, SIDE, SIDE, 128)

    def per_round(shape):
        return [pltpu.VMEM(shape, jnp.float32)] * ROUNDS

    scratch = (
        per_round(tile)
        + per_round((2,) + piece)
        + per_round((4, planes, 128))
        + per_round((2,) + piece)
        + per_round((2,) + piece)
        + per_round((4, planes, 128))
        + per_round((4 * groups,) + piece) * 2
        + per_round((2, 4 * groups, planes, 128)) * 2
        + [pltpu.VMEM(tile, jnp.float32)] * 6
        + [
            pltpu.SemaphoreType.DMA((8,)),
            pltpu.SemaphoreType.DMA((ROUNDS, 8)),
            pltpu.SemaphoreType.DMA((2, 3)),
            pltpu.SemaphoreType.DMA((ROUNDS, 2, 3)),
            pltpu.SemaphoreType.DMA((2, 3, 2)),
            pltpu.SemaphoreType.DMA((ROUNDS, 2, 3, 2)),
        ]
    )
    vmem, smem = pl.BlockSpec(memory_space=pltpu.VMEM), pl.BlockSpec(memory_space=pltpu.SMEM)
    return pl.pallas_call(
        functools.partial(kernel, groups, blocks),
        out_shape=jax.ShapeDtypeStruct(state.shape, jnp.float32),
        in_specs=[smem, smem] + [vmem] * 5,
        out_specs=vmem,
        scratch_shapes=scratch,
        compiler_params=pltpu.CompilerParams(collective_id=0, has_side_effects=True),
    )(nbr_face.T, nbr_edge.T, state, jacobian, metric_diag, metric_cross, coriolis)


def solution(mesh):
    groups, rows, columns = (mesh.shape[axis] for axis in ("face", "fy", "fx"))

    def body(*args):
        state = args[0]
        faces = state.shape[0]
        if rows == columns and rows > 1 and state.shape[1:] == (SIDE, SIDE, 3 * HALF) and faces in (1, 3):
            return fused(groups, rows, *args)
        return per_device(*args)

    return jax.shard_map(
        body,
        mesh=mesh,
        in_specs=(
            P("face", "fy", "fx", None),
            P("face", "fy", "fx"),
            P(None, "face", "fy", "fx"),
            P("face", "fy", "fx"),
            P("face", "fy", "fx"),
            P(),
            P(),
        ),
        out_specs=P("face", "fy", "fx", None),
        check_vma=False,
    )
```
